32 devices in a mesh: rep: 4 (over y, core), shard: 8 (over z, x).
Axes of the slice: x: 2, y: 2, z: 4, core: 2. Of those that a mesh axis runs over, the one named last changes fastest.
Arguments:
- hidden: bfloat16 [14336, 3584], P(('rep', 'shard')), may hold values from -144 to 144
- cotangent: bfloat16 [14336, 1024], P(('rep', 'shard')), may hold values from -6 to 6
- seq_ids: int32 [32, 448], P(('rep', 'shard')), may hold values from 0 to 3, as said below
- response_mask: int32 [32, 448], P(('rep', 'shard')), may hold values from 0 to 1, as said below
- group_ids: int32 [32, 4], P(('rep', 'shard')), may hold values from 0 to 15
- rewards: float32 [32, 4], P(('rep', 'shard')), may hold values from -6 to 6
- new_logp: float32 [32, 448], P(('rep', 'shard')), may hold values from -1.5 to -0.1
- old_logp: float32 [32, 448], P(('rep', 'shard')), may hold values from -1.5 to -0.1
- ref_logp: float32 [32, 448], P(('rep', 'shard')), may hold values from -1.5 to -0.1
- master: float32 [3, 3584, 1024], P(None, 'shard'), may hold values from -6 to 6
Outputs:
- new_master: float32 [3584, 1024], P('shard')
- rollout: bfloat16 [3, 3584, 2048], P(None, None, 'shard')
The draws below stay inside these ranges and needn't reach their ends.
Inputs may be any that keep to these rules, and one draw needn't show every extreme that they name: `seq_ids`: each row numbers its device's 4 sequences in token order, never falling, each with one token or more. `response_mask`: within a sequence, prompt tokens come before response tokens; a sequence may have no response tokens.
All inputs are finite; a program needn't handle non-finite values.
Results may differ from the reference program's by a relative error of at most 0.0095.
Values may be sent and summed in bfloat16 or wider, within the bound.
A program may use at most 128 MiB of HBM per device.

```python
import jax
import jax.numpy as jnp
from jax import lax

D = 3584
HEAD = 128
KV_HEADS = 4
KV = 1024
TP = 8
LAYERS = 3
TOK_DEV = 448
SEQ_DEV = 4
TOKENS = 14336
GROUPS = 16
COPIES = 1
DEVICES = 32


def draw_hidden(key, part):
    column = jnp.arange(D, dtype=jnp.int32).astype(jnp.float32) / (D - 1)
    noise_key = jax.random.fold_in(key, 21)
    base = jnp.clip(jax.random.normal(noise_key, (TOKENS, D), jnp.float32), -6.0, 6.0)
    scale = 1.0 + 5.0 * column
    paired = jax.random.permutation(jax.random.fold_in(key, 22), DEVICES).astype(jnp.int32)
    row_block = jnp.arange(TOKENS, dtype=jnp.int32) // TOK_DEV
    col_block = jnp.arange(D, dtype=jnp.int32) // (D // DEVICES)
    target = paired[row_block]
    spike = jnp.where(target[:, None] == col_block[None, :], 4.0, 1.0)
    return (base * scale[None, :] * spike).astype(jnp.bfloat16)


def sequence_layout(key):
    row_keys = jax.random.split(jax.random.fold_in(key, 11), DEVICES)

    def row_bounds(row_key):
        picked = jax.random.permutation(row_key, TOK_DEV - 1)[:SEQ_DEV - 1] + 1
        return jnp.sort(picked).astype(jnp.int32)
    boundaries = jax.vmap(row_bounds)(row_keys)
    positions = jnp.arange(TOK_DEV, dtype=jnp.int32)
    seq_index = jnp.sum((positions[None, :, None] >= boundaries[:, None, :]).astype(jnp.int32), axis=2).astype(jnp.int32)
    starts = jnp.concatenate([jnp.zeros((DEVICES, 1), jnp.int32), boundaries], axis=1)
    finish = jnp.concatenate([boundaries, jnp.full((DEVICES, 1), TOK_DEV, jnp.int32)], axis=1)
    seq_lengths = finish - starts
    prompt = jax.random.randint(jax.random.fold_in(key, 12), (DEVICES, SEQ_DEV), 0, seq_lengths // 2 + 1).astype(jnp.int32)
    no_reply = jax.random.randint(jax.random.fold_in(key, 13), (DEVICES, SEQ_DEV), 0, 8) == 0
    prompt = jnp.where(no_reply, seq_lengths, prompt)
    tok_start = jnp.take_along_axis(starts, seq_index, axis=1)
    tok_prompt = jnp.take_along_axis(prompt, seq_index, axis=1)
    reply_mask = (positions[None, :] - tok_start >= tok_prompt).astype(jnp.int32)
    return (seq_index, reply_mask)


def draw_seq_ids(key, part):
    return sequence_layout(key)[0]


def draw_response_mask(key, part):
    return sequence_layout(key)[1]


def touch_ends(array, rng, low, largest):
    longest = array.shape.index(max(array.shape))
    spots = []
    for shift in (0, 1):
        where = [jax.random.randint(jax.random.fold_in(rng, axis), (), 0, length) for axis, length in enumerate(array.shape)]
        where[longest] = (where[longest] + shift) % array.shape[longest]
        spots.append(tuple(where))
    return array.at[spots[0]].set(low).at[spots[1]].set(largest)


def steps_of(own_key, dims, pieces, least, top_value):
    level, own = 1.0, jax.random.fold_in(own_key, 6)
    for position, blocks in pieces:
        heights = jnp.exp(jax.random.uniform(jax.random.fold_in(own, position), (blocks,), jnp.float32, least / len(pieces), top_value / len(pieces)))
        level = level * jnp.repeat(heights, dims[position] // blocks).reshape([-1 if axis == position else 1 for axis in range(len(dims))])
    return level


def gaussian(stream_key, shape, scale, reach, shards=(), held_as=jnp.bfloat16):
    level = steps_of(stream_key, shape, shards, -0.22, 0.18) if shards else 1.0
    values = jax.random.normal(stream_key, shape, jnp.float32) * scale * level
    return jnp.minimum(jnp.maximum(values, -reach), reach).astype(held_as)


def setup_inputs(seed: int = 0) -> dict:
    arg_keys = jax.random.split(jax.random.key(seed), 11)
    hidden = draw_hidden(jax.random.fold_in(arg_keys[10], 71), 0)
    cotangent = gaussian(arg_keys[1], (TOKENS, KV), 1.0, 6.0, ((0, 32),))
    seq_ids = draw_seq_ids(jax.random.fold_in(arg_keys[10], 71), 0)
    response_mask = draw_response_mask(jax.random.fold_in(arg_keys[10], 71), 0)
    group_ids = touch_ends(jax.random.randint(arg_keys[4], (DEVICES, SEQ_DEV), 0, GROUPS), jax.random.fold_in(arg_keys[4], 1), 0, GROUPS - 1).astype(jnp.int32)
    rewards = gaussian(arg_keys[5], (DEVICES, SEQ_DEV), 1.0, 6.0, ((0, 32),), jnp.float32)
    new_logp = jnp.clip(-1.5 + 1.4 * jax.random.uniform(arg_keys[6], (DEVICES, TOK_DEV), jnp.float32) ** steps_of(arg_keys[6], (DEVICES, TOK_DEV), ((0, 32),), -0.2, 0.2), -1.5, -0.1)
    old_logp = jnp.clip(-1.5 + 1.4 * jax.random.uniform(arg_keys[7], (DEVICES, TOK_DEV), jnp.float32) ** steps_of(arg_keys[7], (DEVICES, TOK_DEV), ((0, 32),), -0.2, 0.2), -1.5, -0.1)
    ref_logp = jnp.clip(-1.5 + 1.4 * jax.random.uniform(arg_keys[8], (DEVICES, TOK_DEV), jnp.float32) ** steps_of(arg_keys[8], (DEVICES, TOK_DEV), ((0, 32),), -0.2, 0.2), -1.5, -0.1)
    master = gaussian(arg_keys[9], (LAYERS, D, KV), 1.0, 6.0, ((1, 8),), jnp.float32)
    return dict(hidden=hidden, cotangent=cotangent, seq_ids=seq_ids, response_mask=response_mask, group_ids=group_ids, rewards=rewards, new_logp=new_logp, old_logp=old_logp, ref_logp=ref_logp, master=master)


def token_coef(seq_row, mask_row, adv_row, new_row, old_row, ref_row):
    onehot = (seq_row[:, None] == jnp.arange(SEQ_DEV, dtype=jnp.int32)[None, :]).astype(jnp.float32)
    maskf = mask_row.astype(jnp.float32)
    lengths = jnp.maximum(jnp.dot(maskf, onehot, precision=lax.Precision.HIGHEST), 1.0)
    tok_len = jnp.dot(onehot, lengths, precision=lax.Precision.HIGHEST)
    tok_adv = jnp.dot(onehot, adv_row, precision=lax.Precision.HIGHEST)
    surrogate = -tok_adv * jnp.exp(new_row - old_row) + 0.2 * (1.0 - jnp.exp(ref_row - new_row))
    return maskf / tok_len * surrogate

def group_advantage(group_flat, reward_flat, stats):
    groups = stats.shape[1]
    onehot = (group_flat[:, None] == jnp.arange(groups, dtype=jnp.int32)[None, :]).astype(jnp.float32)
    count = jnp.maximum(stats[0], 1.0)
    mean = stats[1] / count
    spread = jnp.sqrt(jnp.maximum(stats[2] / count - mean * mean, 0.0))
    tok_mean = jnp.dot(onehot, mean, precision=lax.Precision.HIGHEST)
    tok_std = jnp.dot(onehot, jnp.maximum(spread, 0.5), precision=lax.Precision.HIGHEST)
    return (reward_flat - tok_mean) / tok_std

def group_sums(group_flat, reward_flat, groups):
    onehot = (group_flat[:, None] == jnp.arange(groups, dtype=jnp.int32)[None, :]).astype(jnp.float32)
    values = jnp.stack([jnp.ones_like(reward_flat), reward_flat, reward_flat * reward_flat], axis=0)
    return jnp.dot(values, onehot, precision=lax.Precision.HIGHEST)

def device_gradient(hidden, delta):
    hidden_rows = hidden.reshape(DEVICES, TOK_DEV, D)
    delta_rows = delta.reshape(DEVICES, TOK_DEV, KV)

    def add_device(running, pair):
        term = lax.dot_general(pair[0], pair[1], (((0,), (0,)), ((), ())), preferred_element_type=jnp.float32)
        partial_value = lax.optimization_barrier(term.astype(jnp.bfloat16))
        return (running + partial_value.astype(jnp.float32), None)
    grad, _ = lax.scan(add_device, jnp.zeros((D, KV), jnp.float32), (hidden_rows, delta_rows))
    return grad

def rollout_layout(layers):
    paired = layers.reshape(LAYERS, D, 2, KV_HEADS, HEAD).transpose(0, 1, 3, 2, 4)
    paired = paired.reshape(LAYERS, D, KV_HEADS, 2 * HEAD)
    by_rank = jnp.repeat(paired, TP // KV_HEADS, axis=2)
    copies = jnp.tile(by_rank, (1, 1, COPIES, 1))
    return copies.reshape(LAYERS, D, COPIES * TP * 2 * HEAD)

def reference(hidden, cotangent, seq_ids, response_mask, group_ids, rewards, new_logp, old_logp, ref_logp, master):
    group_flat = group_ids.reshape(-1)
    reward_flat = rewards.reshape(-1)
    stats = group_sums(group_flat, reward_flat, GROUPS)
    advantage = group_advantage(group_flat, reward_flat, stats).reshape(rewards.shape)
    coef = jax.vmap(token_coef)(seq_ids, response_mask, advantage, new_logp, old_logp, ref_logp)
    delta = (coef.reshape(-1)[:, None] * cotangent.astype(jnp.float32)).astype(jnp.bfloat16)
    grad = device_gradient(hidden, delta)
    rms = jnp.sqrt(jnp.sum(grad * grad) / (D * KV) + 1e-06)
    new_master = master[0] - 0.5 * grad / rms
    layers = jnp.concatenate([new_master[None], master[1:]], axis=0).astype(jnp.bfloat16)
    rollout = rollout_layout(layers)
    return (new_master, rollout)
```

```python
import functools

import jax
import jax.numpy as jnp
from jax import lax
from jax.experimental import pallas as pl
from jax.experimental.pallas import tpu as pltpu
from jax.sharding import PartitionSpec as P

HEAD = 128
KV_HEADS = 4
SEQ_DEV = 4
WIDE = 2 * HEAD
LANES = 128
SUB = 16
MESH = pl.DeviceIdType.MESH


def token_rows(seq_row, mask_row, new_row, old_row, ref_row):
    maskf = mask_row.astype(jnp.float32)
    onehot = [(seq_row == j).astype(jnp.float32) for j in range(SEQ_DEV)]
    tok_len = jnp.zeros_like(maskf)
    for hot in onehot:
        tok_len = tok_len + hot * jnp.maximum(jnp.sum(maskf * hot, axis=1, keepdims=True), 1.0)
    weight = maskf / tok_len
    ratio = -weight * jnp.exp(new_row - old_row)
    return [hot * ratio for hot in onehot] + [weight * (0.2 * (1.0 - jnp.exp(ref_row - new_row)))]


def flip(index, bit):
    step = 1 << bit
    here = (index // step) % 2
    return index + (1 - 2 * here) * step, here


def step_kernel(
    n_rep, n_shard, split, groups, group_hbm, reward_hbm, *args,
):
    token_hbm, args = args[:5], args[5:]
    step_body(n_rep, n_shard, split, groups, group_hbm, reward_hbm, token_hbm, *args)


def step_body(
    n_rep, n_shard, split, groups, group_hbm, reward_hbm, token_hbm,
    hidden_ref, cot_ref, master_ref,
    nm_ref, roll_ref,
    group_ref, reward_ref, ids_in, logp_in, small, stat_in, square_in, info_in, info_own, token_own, token_in, hid, hid_t, cot, delta, part, sums, zin,
    grad, grad_b, base_out, base_in, m0, stage_in, stage_out, rows_in,
    send_sems, recv_sems, local_sems, all_sems, set_send, set_recv,
):
    z_count = n_shard // 2
    dims = n_rep.bit_length() - 1
    everyone = n_rep * n_shard
    r, s = lax.axis_index("rep"), lax.axis_index("shard")
    me = r * n_shard + s
    core, y, x, zi = r % 2, r // 2, s % 2, s // 2
    head = zi % KV_HEADS
    toks, features = hidden_ref.shape
    half = features // 2
    layer_count, rows, cols = master_ref.shape
    sub = rows // split
    final = half // n_rep
    pieces = rows // final
    half_z = z_count // 2
    counter = [0]
    started = []

    def numbered():
        number = counter[0]
        counter[0] += 1
        return number

    def remote(src, dst, device, number, landing=None):
        return pltpu.make_async_remote_copy(
            src_ref=src, dst_ref=dst, send_sem=send_sems.at[number],
            recv_sem=recv_sems.at[number if landing is None else landing],
            device_id=device, device_id_type=MESH)

    def send(src, dst, device):
        copy = remote(src, dst, device, numbered())
        copy.start()
        started.append(copy)
        return copy

    def put(src, dst, device, gone, landed):
        pltpu.make_async_remote_copy(
            src_ref=src, dst_ref=dst, send_sem=set_send.at[gone], recv_sem=set_recv.at[landed],
            device_id=device, device_id_type=MESH).start()

    def whole(ref, number):
        return pltpu.make_async_remote_copy(
            src_ref=ref, dst_ref=ref, send_sem=set_send.at[number], recv_sem=set_recv.at[number],
            device_id=(flip(r, 0)[0], s), device_id_type=MESH)

    def local(src, dst, number):
        copy = pltpu.make_async_copy(src, dst, local_sems.at[number])
        copy.start()
        return copy

    def span(at, size):
        return pl.ds(pl.multiple_of(at, SUB), size)

    def to_all(src, dst, sem):
        @pl.loop(1, everyone)
        def _(i):
            peer = (me + i) % everyone
            pltpu.make_async_remote_copy(
                src_ref=src, dst_ref=dst.at[i - 1], send_sem=all_sems.at[sem], recv_sem=all_sems.at[sem + 1],
                device_id=(peer // n_shard, peer % n_shard), device_id_type=MESH).start()

        return pltpu.make_async_remote_copy(
            src_ref=dst, dst_ref=dst, send_sem=all_sems.at[sem], recv_sem=all_sems.at[sem + 1],
            device_id=(flip(r, 0)[0], s), device_id_type=MESH)

    mate = (flip(r, 0)[0], s)
    options = []
    for bit in range(1, dims):
        other, here = flip(r, bit)
        options.append((other, s, here))
    other, here = flip(s, 0)
    options.append((r, other, here))
    partners, bits = [], []
    for i in range(dims):
        a, b = options[i], options[(i + 1) % dims]
        partners.append(tuple(a[k] + core * (b[k] - a[k]) for k in range(2)))
        bits.append(a[2] + core * (b[2] - a[2]))
    z_peers = [None] + [(r, ((zi + d) % z_count) * 2 + x) for d in range(1, z_count)]

    def home(yy):
        low = yy // pieces
        return low + core * (z_count - 1 - 2 * low), yy % pieces

    def row_of(yy, xx):
        z, piece = home(yy)
        return (2 * z + xx) * rows + piece * final

    def across(yy, xx, i):
        moved = []
        for option in (i % dims, (i + 1) % dims):
            moved.append((flip(yy, option)[0], xx) if option < dims - 1 else (yy, 1 - xx))
        (ya, xa), (yb, xb) = moved
        return ya + core * (yb - ya), xa + core * (xb - xa)

    def spot(j, c):
        low, xx, piece = j // pieces // 2, j // pieces % 2, j % pieces
        yy = (low if c == 0 else half_z - 1 - low) * pieces + piece
        chosen = [(yy >> o) & 1 for o in range(dims - 1)] + [xx]
        return sum(chosen[(i + c) % dims] << (dims - 1 - i) for i in range(dims))

    home_z, home_piece = home(y)
    quarter = r % split
    own_half = pl.ds(pl.multiple_of(core * half, LANES), half)
    other_half = pl.ds(pl.multiple_of((1 - core) * half, LANES), half)
    fetch_stage = local(master_ref.at[pl.ds(1, layer_count - 1), span(quarter * sub, sub), :], stage_in, 0)
    fetch_hid = local(hidden_ref.at[:, own_half], hid.at[pl.ds(0, toks)], 1)
    fetch_cot = local(cot_ref, cot.at[0], 2)
    fetch_m0 = local(master_ref.at[0], m0, 3)
    fetch_small = [local(group_hbm, group_ref, 4), local(reward_hbm, reward_ref, 5)]
    fetch_tokens = [local(ref, ids_in.at[pl.ds(n, 1)], 6 + n) for n, ref in enumerate(token_hbm[:2])]
    fetch_tokens += [local(ref, logp_in.at[pl.ds(n, 1)], 8 + n) for n, ref in enumerate(token_hbm[2:])]

    barrier = pltpu.get_barrier_semaphore()

    @pl.loop(1, everyone)
    def _(i):
        peer = (me + i) % everyone
        pl.semaphore_signal(
            barrier, inc=1, device_id=(peer // n_shard, peer % n_shard), device_id_type=MESH)

    shape = info_in.shape
    line = lax.broadcasted_iota(jnp.int32, shape, 0)
    lane = lax.broadcasted_iota(jnp.int32, shape, 1)
    row_lane = lax.broadcasted_iota(jnp.int32, (1, shape[1]), 1)
    info = jnp.zeros(shape, jnp.float32)
    own_sums = jnp.zeros((1, shape[1]), jnp.float32)
    for copy in fetch_small:
        copy.wait()
    for j in range(SEQ_DEV):
        group, given = group_ref[0, j], reward_ref[0, j]
        info = jnp.where((line == j) & (lane == group), 1.0, info)
        info = jnp.where(line == SEQ_DEV + j, given, info)
        for n, value in enumerate((1.0, given, given * given)):
            own_sums = own_sums + jnp.where(row_lane == n * groups + group, value, 0.0)
    info_own[...] = info
    small[0] = own_sums
    token_own[...] = jnp.zeros_like(token_own)
    with jax.named_scope('w_barrier'):
        pl.semaphore_wait(barrier, everyone - 1)

    stats = to_all(small.at[0], stat_in, 0)
    mate_info = send(info_own, info_in, mate)
    mate_hid = send(hidden_ref.at[:, other_half], hid.at[pl.ds(toks, toks)], mate)
    mate_cot = send(cot_ref, cot.at[1], mate)

    with jax.named_scope('w_stage'):
        fetch_stage.wait()
    for h in range(KV_HEADS):
        low = KV_HEADS * HEAD + h * HEAD
        for l in range(layer_count - 1):
            stage_out[h, l, :, :HEAD] = stage_in[l, :, h * HEAD:(h + 1) * HEAD].astype(jnp.bfloat16)
            stage_out[h, l, :, HEAD:] = stage_in[l, :, low:low + HEAD].astype(jnp.bfloat16)

    def block(z, xx, yy):
        return roll_ref.at[pl.ds(1, layer_count - 1), span((2 * z + xx) * rows + (2 * yy + core) * sub, sub), :]

    yi = quarter // 2
    xy = [(r, flip(s, 0)[0])]
    first_at = (1 - x, yi)
    if split == 4:
        other = flip(r, 1)[0]
        xy = [(r + core * (other - r), s + (1 - core) * (1 - 2 * x)),
              (r + (1 - core) * (other - r), s + core * (1 - 2 * x))]
        first_at = (x + (1 - core) * (1 - 2 * x), yi + core * (1 - 2 * yi))
        second_at = (x + core * (1 - 2 * x), yi + (1 - core) * (1 - 2 * yi))
        third_at = (1 - x, 1 - yi)

    near = [zi]
    for e in range(1, z_count):
        z = zi
        for bit in range(z_count.bit_length() - 1):
            if e >> bit & 1:
                z = flip(z, bit)[0]
        near.append(z)
    m1 = [remote(stage_out.at[near[e] % KV_HEADS], block(zi, x, yi), (r, near[e] * 2 + x), numbered())
          for e in range(1, z_count)]
    for copy in m1:
        copy.start()
        started.append(copy)
    roll_ref[1:, span((2 * zi + x) * rows + quarter * sub, sub), :] = stage_out[head]
    SPREAD_0, SPREAD_1, FORWARD, TO_MATE, GATHER, PIECES, HALVES, GRADS, BASE = range(9)
    level_in = 9

    def spread_block(e):
        if e:
            with jax.named_scope(f'w_m1#{e}'):
                m1[e - 1].wait_recv()
        here = block(near[e], x, yi)
        for n, device in enumerate(xy):
            put(here, here, device, SPREAD_0 + n, SPREAD_0 + n)
        put(here, here, mate, TO_MATE, TO_MATE)

    spread_block(0)

    for copy in fetch_tokens:
        copy.wait()
    terms = token_rows(ids_in[0:1], ids_in[1:2], logp_in[0:1], logp_in[1:2], logp_in[2:3])
    for j, row in enumerate(terms):
        token_own[j:j + 1, :toks] = row
    mate_tok = send(token_own, token_in, mate)

    is_home = home_z == zi
    fetch_m0.wait()

    @pl.when(is_home)
    def _():
        at = span(home_piece * final, final)
        for h in range(KV_HEADS):
            low = KV_HEADS * HEAD + h * HEAD
            base_out[h, :, :HEAD] = m0[at, h * HEAD:(h + 1) * HEAD].astype(jnp.bfloat16)
            base_out[h, :, HEAD:] = m0[at, low:low + HEAD].astype(jnp.bfloat16)
        for d in range(1, z_count):
            put(base_out.at[(head + d) % KV_HEADS], base_in, z_peers[d], BASE, BASE)
        base_in[...] = base_out[head]

    with jax.named_scope('w_hid'):
        fetch_hid.wait()
        mate_hid.wait_recv()

    @pl.loop(0, half // WIDE)
    def _(t):
        at = pl.multiple_of(t * WIDE, WIDE)
        hid_t[pl.ds(at, WIDE), :] = jnp.transpose(hid[:, pl.ds(at, WIDE)])

    with jax.named_scope('w_cot'):
     fetch_cot.wait()
    mate_cot.wait_recv()
    mate_info.wait_recv()
    mate_tok.wait_recv()
    padded = token_own.shape[1]
    tokens = jnp.transpose(jnp.concatenate(
        [token_own[...], token_in[...], jnp.zeros((LANES - 16, padded), jnp.float32)], axis=0))[:toks]

    with jax.named_scope('w_stats'):
        stats.wait_recv()
    total = own_sums + jnp.sum(stat_in[...], axis=0)
    wide = shape[1]
    count = jnp.maximum(total, 1.0)
    mean = pltpu.roll(total, wide - groups, 1) / count
    spread_of = jnp.maximum(
        jnp.sqrt(jnp.maximum(pltpu.roll(total, wide - 2 * groups, 1) / count - mean * mean, 0.0)), 0.5)

    def coef_of(told, low):
        hots, given = told[:SEQ_DEV], told[SEQ_DEV:, 0:1]
        advantage = (given - jnp.sum(hots * mean, axis=1, keepdims=True)) / jnp.sum(
            hots * spread_of, axis=1, keepdims=True)
        out = tokens[:, low + SEQ_DEV:low + SEQ_DEV + 1]
        for j in range(SEQ_DEV):
            out = out + tokens[:, low + j:low + j + 1] * advantage[j:j + 1, :]
        return out

    coefs = [coef_of(info, 0), coef_of(info_in[...], 8)]

    lens, offsets = [half], [0]
    for i in range(dims):
        lens.append(lens[-1] // 2)
        offsets.append(offsets[-1] + bits[i] * lens[-1])
    starts, at = [], 0
    for length in lens[1:]:
        starts.append(at)
        at += length
    turns = [2, 1, 3, 0]
    order = [(head + d) % KV_HEADS for d in turns]
    tile = half // 2
    inbound = {(i, k): numbered() for i in range(dims) for k in range(KV_HEADS)}

    def halves(i, k):
        gone = offsets[i] + (1 - bits[i]) * lens[i + 1]
        return pltpu.make_async_remote_copy(
            src_ref=part.at[order[k], span(gone, lens[i + 1])],
            dst_ref=sums.at[order[k], pl.ds(starts[i], lens[i + 1])],
            send_sem=set_send.at[HALVES], recv_sem=recv_sems.at[inbound[i, k]],
            device_id=partners[i], device_id_type=MESH)

    def pass_on(i, k):
        halves(i, k).start()

    for k in range(KV_HEADS):
        h = order[k]
        for side in range(2):
            low = pl.ds(pl.multiple_of(side * KV_HEADS * HEAD + h * HEAD, HEAD), HEAD)
            for src in range(2):
                delta[src * toks:(src + 1) * toks, side * HEAD:(side + 1) * HEAD] = (
                    coefs[src] * cot[src, :, low].astype(jnp.float32)).astype(jnp.bfloat16)
        for t in range(2):
          with jax.named_scope(f'mul#k={k}'):
            out = jnp.dot(
                hid_t[t * tile:(t + 1) * tile, :], delta[...], preferred_element_type=jnp.float32
            ).astype(jnp.bfloat16)
            for q in range(tile // final):
                j = t * (tile // final) + q
                place = spot(j, 0) + core * (spot(j, 1) - spot(j, 0))
                part[h, span(place * final, final), :] = out[q * final:(q + 1) * final]
        pass_on(0, k)
        if k + 1 < KV_HEADS:
            spread_block(k + 1)
    for e in range(KV_HEADS, z_count):
        spread_block(e)

    inner = min(final, 112)

    def add_in(i, h):
        @pl.loop(0, lens[i + 1] // inner)
        def _(t):
            at = span(offsets[i + 1] + t * inner, inner)
            part[h, at, :] = (
                part[h, at, :].astype(jnp.float32)
                + sums[h, span(starts[i] + t * inner, inner), :].astype(jnp.float32)
            ).astype(jnp.bfloat16)

    last = dims - 1
    mine = span(offsets[dims], final)

    def z_send(k):
        for d in range(1, z_count):
            if d % KV_HEADS == turns[k]:
                put(part.at[order[k], mine], zin.at[d - 1], z_peers[d], GRADS, GRADS)

    for t in range(KV_HEADS + last):
        for i in range(dims):
            k = t - i
            if k < 0 or k >= KV_HEADS:
                continue
            with jax.named_scope(f'w_in#i={i}#k={k}'):
                halves(i, k).wait_recv()
            if i == last and k == KV_HEADS - 1 and z_count == KV_HEADS:
                continue
            add_in(i, order[k])
            if i < last:
                pass_on(i + 1, k)
            else:
                z_send(k)
    with jax.named_scope('w_z'):
        whole(zin, GRADS).wait_recv()

    def gather_sum(t, acc):
        g = part[head, span(offsets[dims] + t * inner, inner), :].astype(jnp.float32)
        if z_count == KV_HEADS:
            g = g + sums[head, span(starts[last] + t * inner, inner), :].astype(jnp.float32)
        at = span(t * inner, inner)
        for d in range(1, z_count):
            g = g + zin[d - 1, at, :].astype(jnp.float32)
        grad[at, :] = g
        grad_b[at, :] = g.astype(jnp.bfloat16)
        return acc + jnp.sum(g * g, axis=0, keepdims=True)

    squares = lax.fori_loop(0, final // inner, gather_sum, jnp.zeros((1, WIDE), jnp.float32))
    own_square = jnp.broadcast_to(jnp.sum(squares, axis=1, keepdims=True), (1, LANES))
    small[1, :, :LANES] = own_square
    all_squares = to_all(small.at[1, :, pl.ds(0, LANES)], square_in, 2)

    nm_numbers = [numbered() for _ in range(n_rep // 2)]
    nm_in = counter[0]
    counter[0] += KV_HEADS * pieces
    nm_copies = []
    for j in range(n_rep // 2):
        copy = remote(
            grad_b, rows_in.at[head, span(home_piece * final, final)], (2 * j + core, 2 * home_z + x),
            nm_numbers[j], nm_in + head * pieces + home_piece)
        leaves = (home_z // KV_HEADS == zi // KV_HEADS) & ((home_z != zi) | (j != y))
        nm_copies.append((leaves, copy))
        pl.when(leaves)(copy.start)

    @pl.when(is_home)
    def _():
        rows_in[head, span(home_piece * final, final), :] = grad_b[...]

    blocks = roll_ref.at[pl.ds(1, layer_count - 1), pl.ds(0, z_count * sub), :]
    with jax.named_scope('w_sp0'):
        whole(blocks, SPREAD_0).wait_recv()
    for z in near:
        got = block(z, *first_at)
        if split == 4:
            put(got, got, xy[1], FORWARD, FORWARD)
        put(got, got, mate, TO_MATE, TO_MATE)

    @pl.when(home_z != zi)
    def _():
        whole(base_in, BASE).wait_recv()

    with jax.named_scope('w_squares'):
        all_squares.wait_recv()
    square = own_square + jnp.sum(square_in[...], axis=0)
    rms = jnp.sqrt(square[:, 0:1] / (features * KV_HEADS * WIDE) + 1e-06)
    scale = 0.5 / rms
    row_me = row_of(y, x)

    @pl.loop(0, final // inner)
    def _(t):
        at = span(t * inner, inner)
        roll_ref[0, span(row_me + t * inner, inner), :] = (
            base_in[at, :].astype(jnp.float32) - scale * grad[at, :]).astype(jnp.bfloat16)

    def layer0(yy, xx):
        return roll_ref.at[0, span(row_of(yy, xx), final), :]

    def gather_in(i):
        return whole(roll_ref.at[0, pl.ds(0, final << (dims - 1 - i)), :], level_in + i)

    have, passed = [(y, x)], 0
    for i in reversed(range(dims)):
        for at in have:
            put(layer0(*at), layer0(*at), partners[i], GATHER, level_in + i)
        for at in have[passed:]:
            put(layer0(*at), layer0(*at), mate, PIECES, PIECES)
        passed = len(have)
        have = have + [across(*at, i) for at in have]
        if i:
            with jax.named_scope(f'w_ag#{i}'):
                gather_in(i).wait_recv()

    keeper = zi // half_z
    pass_number = [numbered() for _ in range(KV_HEADS)]
    hand_over = [remote(rows_in.at[h], rows_in.at[h], mate, pass_number[h]) for h in range(KV_HEADS)]

    def landed(h, p):
        return remote(
            rows_in.at[h, pl.ds(p * final, final)], rows_in.at[h, pl.ds(p * final, final)], mate,
            nm_numbers[0], nm_in + h * pieces + p)

    @pl.when(core == keeper)
    @jax.named_scope('w_rows')
    def _():
        low = zi + core * (z_count - 1 - 2 * zi)
        for h in range(KV_HEADS):
            for p in range(pieces):
                @pl.when((h != head) | (y != low * pieces + p))
                def _():
                    landed(h, p).wait_recv()
            hand_over[h].start()

    if split == 4:
        with jax.named_scope('w_sp1'):
            whole(blocks, SPREAD_1).wait_recv()
        with jax.named_scope('w_fwd'):
            whole(blocks, FORWARD).wait_recv()
        for z in near:
            for there in (second_at, third_at):
                got = block(z, *there)
                put(got, got, mate, TO_MATE, TO_MATE)
    with jax.named_scope('w_gathered'):
        gather_in(0).wait_recv()
    for at in have[passed:]:
        put(layer0(*at), layer0(*at), mate, PIECES, PIECES)

    @pl.when(core != keeper)
    @jax.named_scope('w_hand')
    def _():
        for copy in hand_over:
            copy.wait_recv()

    for h in range(KV_HEADS):
        for side in range(2):
            low = side * KV_HEADS * HEAD + h * HEAD
            nm_ref[:, low:low + HEAD] = (
                m0[:, low:low + HEAD] - scale * rows_in[h, :, side * HEAD:(side + 1) * HEAD].astype(jnp.float32))

    all_blocks = roll_ref.at[pl.ds(1, layer_count - 1), pl.ds(0, z_count * split * sub), :]
    all_pieces = roll_ref.at[0, pl.ds(0, n_rep * final), :]
    with jax.named_scope('w_mate'):
        whole(all_blocks, TO_MATE).wait_recv()
        whole(all_pieces, PIECES).wait_recv()

    @pl.when(core == keeper)
    def _():
        for copy in hand_over:
            copy.wait_send()

    @pl.when(is_home)
    def _():
        whole(zin, BASE).wait_send()

    for leaves, copy in nm_copies:
        pl.when(leaves)(copy.wait_send)
    for copy in started:
        copy.wait_send()
    whole(blocks, SPREAD_0).wait_send()
    if split == 4:
        whole(blocks, SPREAD_1).wait_send()
        whole(blocks, FORWARD).wait_send()
    whole(all_blocks, TO_MATE).wait_send()
    whole(all_pieces, PIECES).wait_send()
    whole(roll_ref.at[0, pl.ds(0, (n_rep - 1) * final), :], GATHER).wait_send()
    whole(part.at[:, pl.ds(0, half - final), :], HALVES).wait_send()
    whole(zin, GRADS).wait_send()
    stats.wait_send()
    all_squares.wait_send()


def per_device(
    n_rep, n_shard, hidden, cotangent, seq_ids, response_mask, group_ids, rewards, new_logp, old_logp, ref_logp,
    master,
):
    everyone = n_rep * n_shard
    groups = everyone * SEQ_DEV // 8
    wide = -(-3 * groups // LANES) * LANES
    toks, features = hidden.shape
    layer_count, rows, cols = master.shape
    z_count = n_shard // 2
    split = 4 if n_rep % 4 == 0 and (rows // 4) % SUB == 0 else 2
    sub = rows // split
    half = features // 2
    final = half // n_rep
    pad = -(-toks // LANES) * LANES
    bf16, f32 = jnp.bfloat16, jnp.float32
    vmem, hbm = pl.BlockSpec(memory_space=pltpu.VMEM), pl.BlockSpec(memory_space=pltpu.HBM)
    sem_count = 96 + 12 * z_count + 6 * n_rep
    return pl.pallas_call(
        functools.partial(step_kernel, n_rep, n_shard, split, groups),
        out_shape=(pltpu.VMEM((rows, cols), f32), pltpu.VMEM((layer_count, features, WIDE), bf16)),
        in_specs=[hbm] * 10,
        out_specs=(vmem, vmem),
        scratch_shapes=[
            pltpu.SMEM((1, SEQ_DEV), jnp.int32),
            pltpu.SMEM((1, SEQ_DEV), f32),
            pltpu.VMEM((2, toks), jnp.int32),
            pltpu.VMEM((3, toks), f32),
            pltpu.VMEM((2, 1, wide), f32),
            pltpu.VMEM((everyone - 1, 1, wide), f32),
            pltpu.VMEM((everyone - 1, 1, LANES), f32),
            pltpu.VMEM((8, wide), f32),
            pltpu.VMEM((8, wide), f32),
            pltpu.VMEM((8, pad), f32),
            pltpu.VMEM((8, pad), f32),
            pltpu.VMEM((2 * toks, half), bf16),
            pltpu.VMEM((half, 2 * toks), bf16),
            pltpu.VMEM((2, toks, cols), bf16),
            pltpu.VMEM((2 * toks, WIDE), bf16),
            pltpu.VMEM((KV_HEADS, half, WIDE), bf16),
            pltpu.VMEM((KV_HEADS, half, WIDE), bf16),
            pltpu.VMEM((z_count - 1, final, WIDE), bf16),
            pltpu.VMEM((final, WIDE), f32),
            pltpu.VMEM((final, WIDE), bf16),
            pltpu.VMEM((KV_HEADS, final, WIDE), bf16),
            pltpu.VMEM((final, WIDE), bf16),
            pltpu.VMEM((rows, cols), f32),
            pltpu.VMEM((layer_count - 1, sub, cols), f32),
            pltpu.VMEM((KV_HEADS, layer_count - 1, sub, WIDE), bf16),
            pltpu.VMEM((KV_HEADS, rows, WIDE), bf16),
            pltpu.SemaphoreType.DMA((sem_count,)),
            pltpu.SemaphoreType.DMA((sem_count,)),
            pltpu.SemaphoreType.DMA((12,)),
            pltpu.SemaphoreType.DMA((4,)),
            pltpu.SemaphoreType.DMA((12 + n_rep,)),
            pltpu.SemaphoreType.DMA((12 + n_rep,)),
        ],
        compiler_params=pltpu.CompilerParams(
            collective_id=0, has_side_effects=True, vmem_limit_bytes=44 * 2**20
        ),
        name="step",
    )(*(pltpu.with_memory_space_constraint(value, pltpu.HBM) for value in (
        group_ids, rewards, seq_ids, response_mask, new_logp, old_logp, ref_logp, hidden, cotangent, master)))


def solution(mesh):
    tokens = P(("rep", "shard"), None)
    return jax.shard_map(
        functools.partial(per_device, mesh.shape["rep"], mesh.shape["shard"]),
        mesh=mesh,
        in_specs=(tokens,) * 9 + (P(None, "shard", None),),
        out_specs=(P("shard", None), P(None, None, "shard")),
        check_vma=False,
    )
```

```python
import functools

import jax
import jax.numpy as jnp
from jax import lax
from jax.experimental import pallas as pl
from jax.experimental.pallas import tpu as pltpu
from jax.sharding import PartitionSpec as P

HEAD = 128
KV_HEADS = 4
SEQ_DEV = 4
WIDE = 2 * HEAD
LANES = 128
SUB = 16
MESH = pl.DeviceIdType.MESH


def token_rows(seq_row, mask_row, new_row, old_row, ref_row):
    maskf = mask_row.astype(jnp.float32)
    onehot = [(seq_row == j).astype(jnp.float32) for j in range(SEQ_DEV)]
    tok_len = jnp.zeros_like(maskf)
    for hot in onehot:
        tok_len = tok_len + hot * jnp.maximum(jnp.sum(maskf * hot, axis=1, keepdims=True), 1.0)
    weight = maskf / tok_len
    ratio = -weight * jnp.exp(new_row - old_row)
    return [hot * ratio for hot in onehot] + [weight * (0.2 * (1.0 - jnp.exp(ref_row - new_row)))]


def flip(index, bit):
    step = 1 << bit
    here = (index // step) % 2
    return index + (1 - 2 * here) * step, here


def step_kernel(
    n_rep, n_shard, split, groups, group_hbm, reward_hbm, *args,
):
    token_hbm, args = args[:5], args[5:]
    step_body(n_rep, n_shard, split, groups, group_hbm, reward_hbm, token_hbm, *args)


def step_body(
    n_rep, n_shard, split, groups, group_hbm, reward_hbm, token_hbm,
    hidden_ref, cot_ref, master_ref,
    nm_ref, roll_ref,
    group_ref, reward_ref, ids_in, logp_in, small, stat_in, square_in, info_in, info_own, token_own, token_in, hid, hid_t, cot, delta, part, sums, zin,
    grad, grad_b, relay_in, base_out, base_in, m0, stage_in, stage_out, rows_in,
    send_sems, recv_sems, local_sems, all_sems, set_send, set_recv,
):
    z_count = n_shard // 2
    dims = n_rep.bit_length() - 1
    everyone = n_rep * n_shard
    r, s = lax.axis_index("rep"), lax.axis_index("shard")
    me = r * n_shard + s
    core, y, x, zi = r % 2, r // 2, s % 2, s // 2
    head = zi % KV_HEADS
    toks, features = hidden_ref.shape
    half = features // 2
    layer_count, rows, cols = master_ref.shape
    sub = rows // split
    final = half // n_rep
    pieces = rows // final
    half_z = z_count // 2
    counter = [0]
    started = []

    def numbered():
        number = counter[0]
        counter[0] += 1
        return number

    def remote(src, dst, device, number, landing=None):
        return pltpu.make_async_remote_copy(
            src_ref=src, dst_ref=dst, send_sem=send_sems.at[number],
            recv_sem=recv_sems.at[number if landing is None else landing],
            device_id=device, device_id_type=MESH)

    def send(src, dst, device):
        copy = remote(src, dst, device, numbered())
        copy.start()
        started.append(copy)
        return copy

    def put(src, dst, device, gone, landed):
        pltpu.make_async_remote_copy(
            src_ref=src, dst_ref=dst, send_sem=set_send.at[gone], recv_sem=set_recv.at[landed],
            device_id=device, device_id_type=MESH).start()

    def whole(ref, number):
        return pltpu.make_async_remote_copy(
            src_ref=ref, dst_ref=ref, send_sem=set_send.at[number], recv_sem=set_recv.at[number],
            device_id=(flip(r, 0)[0], s), device_id_type=MESH)

    def local(src, dst, number):
        copy = pltpu.make_async_copy(src, dst, local_sems.at[number])
        copy.start()
        return copy

    def span(at, size):
        return pl.ds(pl.multiple_of(at, SUB), size)

    def to_all(src, dst, sem):
        @pl.loop(1, everyone)
        def _(i):
            peer = (me + i) % everyone
            pltpu.make_async_remote_copy(
                src_ref=src, dst_ref=dst.at[i - 1], send_sem=all_sems.at[sem], recv_sem=all_sems.at[sem + 1],
                device_id=(peer // n_shard, peer % n_shard), device_id_type=MESH).start()

        return pltpu.make_async_remote_copy(
            src_ref=dst, dst_ref=dst, send_sem=all_sems.at[sem], recv_sem=all_sems.at[sem + 1],
            device_id=(flip(r, 0)[0], s), device_id_type=MESH)

    mate = (flip(r, 0)[0], s)
    options = []
    for bit in range(1, dims):
        other, here = flip(r, bit)
        options.append((other, s, here))
    other, here = flip(s, 0)
    options.append((r, other, here))
    partners, bits = [], []
    for i in range(dims):
        a, b = options[i], options[(i + 1) % dims]
        partners.append(tuple(a[k] + core * (b[k] - a[k]) for k in range(2)))
        bits.append(a[2] + core * (b[2] - a[2]))
    z_peers = [None] + [(r, ((zi + d) % z_count) * 2 + x) for d in range(1, z_count)]

    def home(yy):
        low = yy // pieces
        return low + core * (z_count - 1 - 2 * low), yy % pieces

    def row_of(yy, xx):
        z, piece = home(yy)
        return (2 * z + xx) * rows + piece * final

    def across(yy, xx, i):
        moved = []
        for option in (i % dims, (i + 1) % dims):
            moved.append((flip(yy, option)[0], xx) if option < dims - 1 else (yy, 1 - xx))
        (ya, xa), (yb, xb) = moved
        return ya + core * (yb - ya), xa + core * (xb - xa)

    def spot(j, c):
        low, xx, piece = j // pieces // 2, j // pieces % 2, j % pieces
        yy = (low if c == 0 else half_z - 1 - low) * pieces + piece
        chosen = [(yy >> o) & 1 for o in range(dims - 1)] + [xx]
        return sum(chosen[(i + c) % dims] << (dims - 1 - i) for i in range(dims))

    home_z, home_piece = home(y)
    quarter = r % split
    own_half = pl.ds(pl.multiple_of(core * half, LANES), half)
    other_half = pl.ds(pl.multiple_of((1 - core) * half, LANES), half)
    yi = quarter // 2
    both = 2 if split == 4 else 1
    quarters = [quarter, quarter + (1 - 2 * yi) * 2][:both]
    fetch_stage = [
        local(master_ref.at[pl.ds(1, layer_count - 1), span(q * sub, sub), :], stage_in.at[n], (0, 11)[n])
        for n, q in enumerate(quarters)]
    fetch_hid = local(hidden_ref.at[:, own_half], hid.at[pl.ds(0, toks)], 1)
    fetch_cot = local(cot_ref, cot.at[0], 2)
    fetch_m0 = local(master_ref.at[0], m0, 3)
    fetch_small = [local(group_hbm, group_ref, 4), local(reward_hbm, reward_ref, 5)]
    fetch_tokens = [local(ref, ids_in.at[pl.ds(n, 1)], 6 + n) for n, ref in enumerate(token_hbm[:2])]
    fetch_tokens += [local(ref, logp_in.at[pl.ds(n, 1)], 8 + n) for n, ref in enumerate(token_hbm[2:])]

    barrier = pltpu.get_barrier_semaphore()

    @pl.loop(1, everyone)
    def _(i):
        peer = (me + i) % everyone
        pl.semaphore_signal(
            barrier, inc=1, device_id=(peer // n_shard, peer % n_shard), device_id_type=MESH)

    shape = info_in.shape
    line = lax.broadcasted_iota(jnp.int32, shape, 0)
    lane = lax.broadcasted_iota(jnp.int32, shape, 1)
    row_lane = lax.broadcasted_iota(jnp.int32, (1, shape[1]), 1)
    info = jnp.zeros(shape, jnp.float32)
    own_sums = jnp.zeros((1, shape[1]), jnp.float32)
    for copy in fetch_small:
        copy.wait()
    for j in range(SEQ_DEV):
        group, given = group_ref[0, j], reward_ref[0, j]
        info = jnp.where((line == j) & (lane == group), 1.0, info)
        info = jnp.where(line == SEQ_DEV + j, given, info)
        for n, value in enumerate((1.0, given, given * given)):
            own_sums = own_sums + jnp.where(row_lane == n * groups + group, value, 0.0)
    info_own[...] = info
    small[0] = own_sums
    token_own[...] = jnp.zeros_like(token_own)
    with jax.named_scope('w_barrier'):
        pl.semaphore_wait(barrier, everyone - 1)

    stats = to_all(small.at[0], stat_in, 0)
    mate_info = send(info_own, info_in, mate)
    mate_hid = send(hidden_ref.at[:, other_half], hid.at[pl.ds(toks, toks)], mate)
    mate_cot = send(cot_ref, cot.at[1], mate)

    def block(z, xx, yy):
        return roll_ref.at[pl.ds(1, layer_count - 1), span((2 * z + xx) * rows + (2 * yy + core) * sub, sub), :]

    near = [zi]
    for e in range(1, z_count):
        z = zi
        for bit in range(z_count.bit_length() - 1):
            if e >> bit & 1:
                z = flip(z, bit)[0]
        near.append(z)
    beside = (r, flip(s, 0)[0])
    above = (flip(r, 1)[0], s)
    halves_at = [yi, 1 - yi]
    m1 = []
    for n in range(both):
        with jax.named_scope('w_stage'):
            fetch_stage[n].wait()
        for h in range(KV_HEADS):
            low = KV_HEADS * HEAD + h * HEAD
            for l in range(layer_count - 1):
                stage_out[n, h, l, :, :HEAD] = stage_in[n, l, :, h * HEAD:(h + 1) * HEAD].astype(jnp.bfloat16)
                stage_out[n, h, l, :, HEAD:] = stage_in[n, l, :, low:low + HEAD].astype(jnp.bfloat16)
        m1.append([send(stage_out.at[n, near[e] % KV_HEADS], block(zi, x, halves_at[n]), (r, near[e] * 2 + x))
                   for e in range(1, z_count)])
        roll_ref[1:, span((2 * zi + x) * rows + quarters[n] * sub, sub), :] = stage_out[n, head]

    SPREAD, FORWARD, TO_MATE, GATHER, PIECES, HALVES, GRADS, BASE, RELAY = range(9)
    level_in = 9

    spread_in = [numbered() for _ in range(z_count)]

    def spread_copy(e):
        here = block(near[e], x, yi)
        return pltpu.make_async_remote_copy(
            src_ref=here, dst_ref=here, send_sem=set_send.at[SPREAD], recv_sem=recv_sems.at[spread_in[e]],
            device_id=beside, device_id_type=MESH)

    def spread_block(e):
        if e:
            with jax.named_scope(f'w_m1#{e}'):
                m1[0][e - 1].wait_recv()
        spread_copy(e).start()
        here = block(near[e], x, yi)
        put(here, here, mate, TO_MATE, TO_MATE)
        if e == 0 and both == 2:
            here = block(zi, x, 1 - yi)
            put(here, here, beside, FORWARD, FORWARD)

    def forward_block(e):
        with jax.named_scope(f'w_sp#{e}'):
            spread_copy(e).wait_recv()
        got = block(near[e], 1 - x, yi)
        if both == 2 and e:
            put(got, got, above, FORWARD, FORWARD)
        put(got, got, mate, TO_MATE, TO_MATE)

    spread_block(0)

    for copy in fetch_tokens:
        copy.wait()
    terms = token_rows(ids_in[0:1], ids_in[1:2], logp_in[0:1], logp_in[1:2], logp_in[2:3])
    for j, row in enumerate(terms):
        token_own[j:j + 1, :toks] = row
    mate_tok = send(token_own, token_in, mate)

    is_home = home_z == zi
    fetch_m0.wait()

    @pl.when(is_home)
    def _():
        at = span(home_piece * final, final)
        for h in range(KV_HEADS):
            low = KV_HEADS * HEAD + h * HEAD
            base_out[h, :, :HEAD] = m0[at, h * HEAD:(h + 1) * HEAD].astype(jnp.bfloat16)
            base_out[h, :, HEAD:] = m0[at, low:low + HEAD].astype(jnp.bfloat16)
        for d in range(1, z_count):
            put(base_out.at[(head + d) % KV_HEADS], base_in, z_peers[d], BASE, BASE)
        base_in[...] = base_out[head]

    with jax.named_scope('w_hid'):
        fetch_hid.wait()
        mate_hid.wait_recv()

    @pl.loop(0, half // WIDE)
    def _(t):
        at = pl.multiple_of(t * WIDE, WIDE)
        hid_t[pl.ds(at, WIDE), :] = jnp.transpose(hid[:, pl.ds(at, WIDE)])

    with jax.named_scope('w_cot'):
     fetch_cot.wait()
    mate_cot.wait_recv()
    mate_info.wait_recv()
    mate_tok.wait_recv()
    padded = token_own.shape[1]
    tokens = jnp.transpose(jnp.concatenate(
        [token_own[...], token_in[...], jnp.zeros((LANES - 16, padded), jnp.float32)], axis=0))[:toks]

    spread_block(1)
    with jax.named_scope('w_stats'):
        stats.wait_recv()
    total = own_sums + jnp.sum(stat_in[...], axis=0)
    wide = shape[1]
    count = jnp.maximum(total, 1.0)
    mean = pltpu.roll(total, wide - groups, 1) / count
    spread_of = jnp.maximum(
        jnp.sqrt(jnp.maximum(pltpu.roll(total, wide - 2 * groups, 1) / count - mean * mean, 0.0)), 0.5)

    def coef_of(told, low):
        hots, given = told[:SEQ_DEV], told[SEQ_DEV:, 0:1]
        advantage = (given - jnp.sum(hots * mean, axis=1, keepdims=True)) / jnp.sum(
            hots * spread_of, axis=1, keepdims=True)
        out = tokens[:, low + SEQ_DEV:low + SEQ_DEV + 1]
        for j in range(SEQ_DEV):
            out = out + tokens[:, low + j:low + j + 1] * advantage[j:j + 1, :]
        return out

    coefs = [coef_of(info, 0), coef_of(info_in[...], 8)]

    lens, offsets = [half], [0]
    for i in range(dims):
        lens.append(lens[-1] // 2)
        offsets.append(offsets[-1] + bits[i] * lens[-1])
    starts, at = [], 0
    for length in lens[1:]:
        starts.append(at)
        at += length
    turns = [2, 1, 3, 0]
    order = [(head + d) % KV_HEADS for d in turns]
    tile = half // 2
    chunks = 2 * KV_HEADS
    inbound = {(i, k): numbered() for i in range(dims) for k in range(chunks)}

    def halves(i, k):
        gone = offsets[i] + (1 - bits[i]) * lens[i + 1]
        return pltpu.make_async_remote_copy(
            src_ref=part.at[order[k // 2], k % 2, span(gone, lens[i + 1])],
            dst_ref=sums.at[order[k // 2], k % 2, pl.ds(starts[i], lens[i + 1])],
            send_sem=set_send.at[HALVES], recv_sem=recv_sems.at[inbound[i, k]],
            device_id=partners[i], device_id_type=MESH)

    def pass_on(i, k):
        halves(i, k).start()

    for k in range(KV_HEADS):
        h = order[k]
        for side in range(2):
            low = pl.ds(pl.multiple_of(side * KV_HEADS * HEAD + h * HEAD, HEAD), HEAD)
            for src in range(2):
                delta[src * toks:(src + 1) * toks, side * HEAD:(side + 1) * HEAD] = (
                    coefs[src] * cot[src, :, low].astype(jnp.float32)).astype(jnp.bfloat16)
        for t in range(2):
          with jax.named_scope(f'mul#k={k}'):
            out = jnp.dot(
                hid_t[t * tile:(t + 1) * tile, :], delta[...], preferred_element_type=jnp.float32
            ).astype(jnp.bfloat16)
            for q in range(tile // final):
                j = t * (tile // final) + q
                place = spot(j, 0) + core * (spot(j, 1) - spot(j, 0))
                for side in range(2):
                    part[h, side, span(place * final, final), :] = (
                        out[q * final:(q + 1) * final, side * HEAD:(side + 1) * HEAD])
        pass_on(0, 2 * k)
        pass_on(0, 2 * k + 1)
        if k in (1, 2) and k + 1 < z_count:
            spread_block(k + 1)
    for e in range(KV_HEADS, z_count):
        spread_block(e)

    inner = min(final, 112)

    def add_in(i, k):
        h, side = order[k // 2], k % 2

        @pl.loop(0, lens[i + 1] // inner)
        def _(t):
            at = span(offsets[i + 1] + t * inner, inner)
            part[h, side, at, :] = (
                part[h, side, at, :].astype(jnp.float32)
                + sums[h, side, span(starts[i] + t * inner, inner), :].astype(jnp.float32)
            ).astype(jnp.bfloat16)

    last = dims - 1
    mine = span(offsets[dims], final)
    z_in = {(d, side): numbered() for side in range(2) for d in range(1, z_count)}

    def z_copy(d, side):
        return pltpu.make_async_remote_copy(
            src_ref=part.at[(head + d) % KV_HEADS, side, mine], dst_ref=zin.at[d - 1, side],
            send_sem=set_send.at[GRADS], recv_sem=recv_sems.at[z_in[d, side]],
            device_id=z_peers[d], device_id_type=MESH)

    def z_send(k):
        for d in range(1, z_count):
            if d % KV_HEADS == turns[k // 2]:
                z_copy(d, k % 2).start()

    far = z_count > KV_HEADS
    for t in range(chunks + last):
        for i in range(dims):
            k = t - i
            if k < 0 or k >= chunks:
                continue
            with jax.named_scope(f'w_in#i={i}#k={k}'):
                halves(i, k).wait_recv()
            if i == last and k // 2 == KV_HEADS - 1 and not far:
                side = k % 2
                grad[:, side * HEAD:(side + 1) * HEAD] = (
                    part[head, side, mine, :].astype(jnp.float32)
                    + sums[head, side, pl.ds(starts[last], final), :].astype(jnp.float32))
                continue
            add_in(i, k)
            if i < last:
                pass_on(i + 1, k)
            else:
                z_send(k)
        if t == 2:
            forward_block(0)
            forward_block(1)
        if t == 6 and z_count > 2:
            forward_block(2)
    if far:
        for side in range(2):
            grad[:, side * HEAD:(side + 1) * HEAD] = part[head, side, mine, :].astype(jnp.float32)

    arrivals = [d for turn in turns for d in range(1, z_count) if d % KV_HEADS == turn]
    own_square = jnp.zeros((1, HEAD), jnp.float32)
    for d in arrivals:
        for side in range(2):
            with jax.named_scope(f'w_z#{d}'):
                z_copy(d, side).wait_recv()
            cut = slice(side * HEAD, (side + 1) * HEAD)
            g = grad[:, cut] + zin[d - 1, side].astype(jnp.float32)
            grad[:, cut] = g
            if d == arrivals[-1]:
                own_square = own_square + jnp.sum(g * g, axis=0, keepdims=True)
                grad_b[:, cut] = g.astype(jnp.bfloat16)

    own_square = jnp.broadcast_to(jnp.sum(own_square, axis=1, keepdims=True), (1, LANES))
    small[1, :, :LANES] = own_square
    all_squares = to_all(small.at[1, :, pl.ds(0, LANES)], square_in, 2)

    relayed = n_rep == 4 and pieces == 1
    y_other = flip(y, 0)[0] if relayed else y
    other_z = home(y_other)[0]
    nm_numbers = [numbered() for _ in range(n_rep // 2)]
    nm_in = counter[0]
    counter[0] += KV_HEADS * pieces
    here_rows = rows_in.at[head, span(home_piece * final, final)]
    if relayed:
        put(grad_b, relay_in, above, RELAY, RELAY)
        nm_copies = [
            (home_z != zi, remote(grad_b, here_rows, (r, 2 * home_z + x), nm_numbers[0], nm_in + head)),
            (other_z != zi, remote(relay_in, here_rows, (r, 2 * other_z + x), nm_numbers[1], nm_in + head))]
        pl.when(home_z != zi)(nm_copies[0][1].start)
    else:
        nm_copies = []
        for j in range(n_rep // 2):
            copy = remote(
                grad_b, here_rows, (2 * j + core, 2 * home_z + x),
                nm_numbers[j], nm_in + head * pieces + home_piece)
            leaves = (home_z // KV_HEADS == zi // KV_HEADS) & ((home_z != zi) | (j != y))
            nm_copies.append((leaves, copy))
            pl.when(leaves)(copy.start)

    @pl.when(is_home)
    def _():
        rows_in[head, span(home_piece * final, final), :] = grad_b[...]

    for e in range(3 if z_count > 2 else 2, z_count):
        forward_block(e)
    if both == 2:
        for e in range(z_count):
            if e:
                m1[1][e - 1].wait_recv()
            got = block(near[e], x, 1 - yi)
            put(got, got, mate, TO_MATE, TO_MATE)

    @pl.when(home_z != zi)
    def _():
        whole(base_in, BASE).wait_recv()

    with jax.named_scope('w_squares'):
        all_squares.wait_recv()
    square = own_square + jnp.sum(square_in[...], axis=0)
    rms = jnp.sqrt(square[:, 0:1] / (features * KV_HEADS * WIDE) + 1e-06)
    scale = 0.5 / rms
    row_me = row_of(y, x)

    @pl.loop(0, final // inner)
    def _(t):
        at = span(t * inner, inner)
        roll_ref[0, span(row_me + t * inner, inner), :] = (
            base_in[at, :].astype(jnp.float32) - scale * grad[at, :]).astype(jnp.bfloat16)

    def layer0(yy, xx):
        return roll_ref.at[0, span(row_of(yy, xx), final), :]

    def gather_in(i):
        return whole(roll_ref.at[0, pl.ds(0, final << (dims - 1 - i)), :], level_in + i)

    have, passed = [(y, x)], 0
    for i in reversed(range(dims)):
        for at in have:
            put(layer0(*at), layer0(*at), partners[i], GATHER, level_in + i)
        for at in have[passed:]:
            put(layer0(*at), layer0(*at), mate, PIECES, PIECES)
        passed = len(have)
        have = have + [across(*at, i) for at in have]
        if i == last and relayed:
            with jax.named_scope('w_relay'):
                whole(relay_in, RELAY).wait_recv()
            pl.when(other_z != zi)(nm_copies[1][1].start)

            @pl.when(other_z == zi)
            def _():
                rows_in[head] = relay_in[...]
        if i:
            with jax.named_scope(f'w_ag#{i}'):
                gather_in(i).wait_recv()

    keeper = zi // half_z
    pass_number = [numbered() for _ in range(KV_HEADS)]
    hand_over = [remote(rows_in.at[h], rows_in.at[h], mate, pass_number[h]) for h in range(KV_HEADS)]

    def landed(h, p):
        return remote(
            rows_in.at[h, pl.ds(p * final, final)], rows_in.at[h, pl.ds(p * final, final)], mate,
            nm_numbers[0], nm_in + h * pieces + p)

    @pl.when(core == keeper)
    @jax.named_scope('w_rows')
    def _():
        low = zi + core * (z_count - 1 - 2 * zi)
        for h in range(KV_HEADS):
            for p in range(pieces):
                @pl.when((h != head) if relayed else (h != head) | (y != low * pieces + p))
                def _():
                    landed(h, p).wait_recv()
            hand_over[h].start()

    blocks = roll_ref.at[pl.ds(1, layer_count - 1), pl.ds(0, z_count * sub), :]
    if both == 2:
        with jax.named_scope('w_fwd'):
            whole(blocks, FORWARD).wait_recv()
        for z in near:
            got = block(z, 1 - x, 1 - yi)
            put(got, got, mate, TO_MATE, TO_MATE)
    with jax.named_scope('w_gathered'):
        gather_in(0).wait_recv()
    for at in have[passed:]:
        put(layer0(*at), layer0(*at), mate, PIECES, PIECES)

    @pl.when(core != keeper)
    @jax.named_scope('w_hand')
    def _():
        for copy in hand_over:
            copy.wait_recv()

    for h in range(KV_HEADS):
        for side in range(2):
            low = side * KV_HEADS * HEAD + h * HEAD
            nm_ref[:, low:low + HEAD] = (
                m0[:, low:low + HEAD] - scale * rows_in[h, :, side * HEAD:(side + 1) * HEAD].astype(jnp.float32))

    all_blocks = roll_ref.at[pl.ds(1, layer_count - 1), pl.ds(0, z_count * split * sub), :]
    all_pieces = roll_ref.at[0, pl.ds(0, n_rep * final), :]
    with jax.named_scope('w_mate'):
        whole(all_blocks, TO_MATE).wait_recv()
        whole(all_pieces, PIECES).wait_recv()

    @pl.when(core == keeper)
    def _():
        for copy in hand_over:
            copy.wait_send()

    @pl.when(is_home)
    def _():
        whole(zin, BASE).wait_send()

    for leaves, copy in nm_copies:
        pl.when(leaves)(copy.wait_send)
    for copy in started:
        copy.wait_send()
    whole(blocks, SPREAD).wait_send()
    if both == 2:
        whole(blocks, FORWARD).wait_send()
    if relayed:
        whole(relay_in, RELAY).wait_send()
    whole(all_blocks, TO_MATE).wait_send()
    whole(all_pieces, PIECES).wait_send()
    whole(roll_ref.at[0, pl.ds(0, (n_rep - 1) * final), :], GATHER).wait_send()
    whole(part.at[:, :, pl.ds(0, half - final), :], HALVES).wait_send()
    whole(zin, GRADS).wait_send()
    stats.wait_send()
    all_squares.wait_send()


def per_device(
    n_rep, n_shard, hidden, cotangent, seq_ids, response_mask, group_ids, rewards, new_logp, old_logp, ref_logp,
    master,
):
    everyone = n_rep * n_shard
    groups = everyone * SEQ_DEV // 8
    wide = -(-3 * groups // LANES) * LANES
    toks, features = hidden.shape
    layer_count, rows, cols = master.shape
    z_count = n_shard // 2
    split = 4 if n_rep % 4 == 0 and (rows // 4) % SUB == 0 else 2
    sub = rows // split
    half = features // 2
    final = half // n_rep
    pad = -(-toks // LANES) * LANES
    bf16, f32 = jnp.bfloat16, jnp.float32
    vmem, hbm = pl.BlockSpec(memory_space=pltpu.VMEM), pl.BlockSpec(memory_space=pltpu.HBM)
    sem_count = 96 + 12 * z_count + 6 * n_rep
    return pl.pallas_call(
        functools.partial(step_kernel, n_rep, n_shard, split, groups),
        out_shape=(pltpu.VMEM((rows, cols), f32), pltpu.VMEM((layer_count, features, WIDE), bf16)),
        in_specs=[hbm] * 10,
        out_specs=(vmem, vmem),
        scratch_shapes=[
            pltpu.SMEM((1, SEQ_DEV), jnp.int32),
            pltpu.SMEM((1, SEQ_DEV), f32),
            pltpu.VMEM((2, toks), jnp.int32),
            pltpu.VMEM((3, toks), f32),
            pltpu.VMEM((2, 1, wide), f32),
            pltpu.VMEM((everyone - 1, 1, wide), f32),
            pltpu.VMEM((everyone - 1, 1, LANES), f32),
            pltpu.VMEM((8, wide), f32),
            pltpu.VMEM((8, wide), f32),
            pltpu.VMEM((8, pad), f32),
            pltpu.VMEM((8, pad), f32),
            pltpu.VMEM((2 * toks, half), bf16),
            pltpu.VMEM((half, 2 * toks), bf16),
            pltpu.VMEM((2, toks, cols), bf16),
            pltpu.VMEM((2 * toks, WIDE), bf16),
            pltpu.VMEM((KV_HEADS, 2, half, HEAD), bf16),
            pltpu.VMEM((KV_HEADS, 2, half, HEAD), bf16),
            pltpu.VMEM((z_count - 1, 2, final, HEAD), bf16),
            pltpu.VMEM((final, WIDE), f32),
            pltpu.VMEM((final, WIDE), bf16),
            pltpu.VMEM((final, WIDE), bf16),
            pltpu.VMEM((KV_HEADS, final, WIDE), bf16),
            pltpu.VMEM((final, WIDE), bf16),
            pltpu.VMEM((rows, cols), f32),
            pltpu.VMEM((2, layer_count - 1, sub, cols), f32),
            pltpu.VMEM((2, KV_HEADS, layer_count - 1, sub, WIDE), bf16),
            pltpu.VMEM((KV_HEADS, rows, WIDE), bf16),
            pltpu.SemaphoreType.DMA((sem_count,)),
            pltpu.SemaphoreType.DMA((sem_count,)),
            pltpu.SemaphoreType.DMA((12,)),
            pltpu.SemaphoreType.DMA((4,)),
            pltpu.SemaphoreType.DMA((12 + n_rep,)),
            pltpu.SemaphoreType.DMA((12 + n_rep,)),
        ],
        compiler_params=pltpu.CompilerParams(
            collective_id=0, has_side_effects=True, vmem_limit_bytes=44 * 2**20
        ),
        name="step",
    )(*(pltpu.with_memory_space_constraint(value, pltpu.HBM) for value in (
        group_ids, rewards, seq_ids, response_mask, new_logp, old_logp, ref_logp, hidden, cotangent, master)))


def solution(mesh):
    tokens = P(("rep", "shard"), None)
    return jax.shard_map(
        functools.partial(per_device, mesh.shape["rep"], mesh.shape["shard"]),
        mesh=mesh,
        in_specs=(tokens,) * 9 + (P(None, "shard", None),),
        out_specs=(P("shard", None), P(None, None, "shard")),
        check_vma=False,
    )
```

```python
import functools

import jax
import jax.numpy as jnp
from jax import lax
from jax.experimental import pallas as pl
from jax.experimental.pallas import tpu as pltpu
from jax.sharding import PartitionSpec as P

HEAD = 128
KV_HEADS = 4
SEQ_DEV = 4
WIDE = 2 * HEAD
LANES = 128
SUB = 16
MESH = pl.DeviceIdType.MESH


def token_rows(seq_row, mask_row, new_row, old_row, ref_row):
    maskf = mask_row.astype(jnp.float32)
    onehot = [(seq_row == j).astype(jnp.float32) for j in range(SEQ_DEV)]
    tok_len = jnp.zeros_like(maskf)
    for hot in onehot:
        tok_len = tok_len + hot * jnp.maximum(jnp.sum(maskf * hot, axis=1, keepdims=True), 1.0)
    weight = maskf / tok_len
    ratio = -weight * jnp.exp(new_row - old_row)
    return [hot * ratio for hot in onehot] + [weight * (0.2 * (1.0 - jnp.exp(ref_row - new_row)))]


def flip(index, bit):
    step = 1 << bit
    here = (index // step) % 2
    return index + (1 - 2 * here) * step, here


def step_kernel(
    n_rep, n_shard, split, groups, group_hbm, reward_hbm, *args,
):
    token_hbm, args = args[:5], args[5:]
    step_body(n_rep, n_shard, split, groups, group_hbm, reward_hbm, token_hbm, *args)


def step_body(
    n_rep, n_shard, split, groups, group_hbm, reward_hbm, token_hbm,
    hidden_ref, cot_ref, master_ref,
    nm_ref, roll_ref,
    group_ref, reward_ref, ids_in, logp_in, small, stat_in, square_in, info_in, info_own, token_own, token_in, hid, hid_t, cot, delta, part, sums, zin,
    grad, grad_b, relay_in, base_out, base_in, m0, stage_in, stage_out, rows_in,
    local_sems, all_sems, set_send, set_recv,
):
    z_count = n_shard // 2
    dims = n_rep.bit_length() - 1
    everyone = n_rep * n_shard
    r, s = lax.axis_index("rep"), lax.axis_index("shard")
    me = r * n_shard + s
    core, y, x, zi = r % 2, r // 2, s % 2, s // 2
    head = zi % KV_HEADS
    toks, features = hidden_ref.shape
    half = features // 2
    layer_count, rows, cols = master_ref.shape
    sub = rows // split
    final = half // n_rep
    pieces = rows // final
    half_z = z_count // 2
    counter = [0]
    (SPREAD, FORWARD, TO_MATE, PIECES, BASE, RELAY, HAND,
     MASTERS, GATHER, HALVES, GRADS, RETURN) = range(12)
    given_in, given_out = 7, 12
    mate = (flip(r, 0)[0], s)

    def numbered():
        number = given_in + counter[0]
        counter[0] += 1
        return number

    def copy_to(src, dst, device, gone, landed):
        return pltpu.make_async_remote_copy(
            src_ref=src, dst_ref=dst, send_sem=set_send.at[gone], recv_sem=set_recv.at[landed],
            device_id=device, device_id_type=MESH)

    def put(src, dst, device, gone, landed):
        copy_to(src, dst, device, gone, landed).start()

    def whole(ref, number):
        return copy_to(ref, ref, mate, number, number)

    def landing(ref, number):
        return copy_to(ref, ref, mate, 0, number)

    def local(src, dst, number):
        copy = pltpu.make_async_copy(src, dst, local_sems.at[number])
        copy.start()
        return copy

    def span(at, size):
        return pl.ds(pl.multiple_of(at, SUB), size)

    def to_all(src, dst, sem):
        @pl.loop(1, everyone)
        def _(i):
            peer = (me + i) % everyone
            pltpu.make_async_remote_copy(
                src_ref=src, dst_ref=dst.at[i - 1], send_sem=all_sems.at[sem], recv_sem=all_sems.at[sem + 1],
                device_id=(peer // n_shard, peer % n_shard), device_id_type=MESH).start()

        return pltpu.make_async_remote_copy(
            src_ref=dst, dst_ref=dst, send_sem=all_sems.at[sem], recv_sem=all_sems.at[sem + 1],
            device_id=(flip(r, 0)[0], s), device_id_type=MESH)

    options = []
    for bit in range(1, dims):
        other, here = flip(r, bit)
        options.append((other, s, here))
    other, here = flip(s, 0)
    options.append((r, other, here))
    partners, bits = [], []
    for i in range(dims):
        a, b = options[i], options[(i + 1) % dims]
        partners.append(tuple(a[k] + core * (b[k] - a[k]) for k in range(2)))
        bits.append(a[2] + core * (b[2] - a[2]))
    z_peers = [None] + [(r, ((zi + d) % z_count) * 2 + x) for d in range(1, z_count)]

    def home(yy):
        low = yy // pieces
        return low + core * (z_count - 1 - 2 * low), yy % pieces

    def row_of(yy, xx):
        z, piece = home(yy)
        return (2 * z + xx) * rows + piece * final

    def across(yy, xx, i):
        moved = []
        for option in (i % dims, (i + 1) % dims):
            moved.append((flip(yy, option)[0], xx) if option < dims - 1 else (yy, 1 - xx))
        (ya, xa), (yb, xb) = moved
        return ya + core * (yb - ya), xa + core * (xb - xa)

    def spot(j, c):
        low, xx, piece = j // pieces // 2, j // pieces % 2, j % pieces
        yy = (low if c == 0 else half_z - 1 - low) * pieces + piece
        chosen = [(yy >> o) & 1 for o in range(dims - 1)] + [xx]
        return sum(chosen[(i + c) % dims] << (dims - 1 - i) for i in range(dims))

    home_z, home_piece = home(y)
    quarter = r % split
    own_half = pl.ds(pl.multiple_of(core * half, LANES), half)
    other_half = pl.ds(pl.multiple_of((1 - core) * half, LANES), half)
    yi = quarter // 2
    both = 2 if split == 4 else 1
    quarters = [quarter, quarter + (1 - 2 * yi) * 2][:both]
    fetch_stage = [
        local(master_ref.at[pl.ds(1, layer_count - 1), span(q * sub, sub), :], stage_in.at[n], (0, 11)[n])
        for n, q in enumerate(quarters)]
    fetch_hid = local(hidden_ref.at[:, own_half], hid.at[pl.ds(0, toks)], 1)
    fetch_cot = local(cot_ref, cot.at[0], 2)
    fetch_m0 = local(master_ref.at[0], m0, 3)
    fetch_small = [local(group_hbm, group_ref, 4), local(reward_hbm, reward_ref, 5)]
    fetch_tokens = [local(ref, ids_in.at[pl.ds(n, 1)], 6 + n) for n, ref in enumerate(token_hbm[:2])]
    fetch_tokens += [local(ref, logp_in.at[pl.ds(n, 1)], 8 + n) for n, ref in enumerate(token_hbm[2:])]

    barrier = pltpu.get_barrier_semaphore()

    @pl.loop(1, everyone)
    def _(i):
        peer = (me + i) % everyone
        pl.semaphore_signal(
            barrier, inc=1, device_id=(peer // n_shard, peer % n_shard), device_id_type=MESH)

    shape = info_in.shape
    line = lax.broadcasted_iota(jnp.int32, shape, 0)
    lane = lax.broadcasted_iota(jnp.int32, shape, 1)
    row_lane = lax.broadcasted_iota(jnp.int32, (1, shape[1]), 1)
    info = jnp.zeros(shape, jnp.float32)
    own_sums = jnp.zeros((1, shape[1]), jnp.float32)
    for copy in fetch_small:
        copy.wait()
    for j in range(SEQ_DEV):
        group, given = group_ref[0, j], reward_ref[0, j]
        info = jnp.where((line == j) & (lane == group), 1.0, info)
        info = jnp.where(line == SEQ_DEV + j, given, info)
        for n, value in enumerate((1.0, given, given * given)):
            own_sums = own_sums + jnp.where(row_lane == n * groups + group, value, 0.0)
    info_own[...] = info
    small[0] = own_sums
    token_own[...] = jnp.zeros_like(token_own)
    with jax.named_scope('w_barrier'):
        pl.semaphore_wait(barrier, everyone - 1)

    stats = to_all(small.at[0], stat_in, 0)
    sent_out = n_rep // 2 + given_out
    mate_copies = [
        copy_to(src, dst, mate, sent_out + n, numbered()) for n, (src, dst) in enumerate((
            (info_own, info_in), (hidden_ref.at[:, other_half], hid.at[pl.ds(toks, toks)]), (cot_ref, cot.at[1]),
            (token_own, token_in)))]
    mate_info, mate_hid, mate_cot, mate_tok = mate_copies
    for copy in mate_copies[:3]:
        copy.start()

    def block(z, xx, yy):
        return roll_ref.at[pl.ds(1, layer_count - 1), span((2 * z + xx) * rows + (2 * yy + core) * sub, sub), :]

    near = [zi]
    for e in range(1, z_count):
        z = zi
        for bit in range(z_count.bit_length() - 1):
            if e >> bit & 1:
                z = flip(z, bit)[0]
        near.append(z)
    beside = (r, flip(s, 0)[0])
    above = (flip(r, 1)[0], s)
    halves_at = [yi, 1 - yi]
    m1 = [[numbered() for _ in range(1, z_count)] for _ in range(both)]

    def master_in(n, e):
        return landing(block(zi, x, halves_at[n]), m1[n][e - 1])

    def stage_masters(n):
        with jax.named_scope('w_stage'):
            fetch_stage[n].wait()
        for h in range(KV_HEADS):
            low = KV_HEADS * HEAD + h * HEAD
            for l in range(layer_count - 1):
                stage_out[n, h, l, :, :HEAD] = stage_in[n, l, :, h * HEAD:(h + 1) * HEAD].astype(jnp.bfloat16)
                stage_out[n, h, l, :, HEAD:] = stage_in[n, l, :, low:low + HEAD].astype(jnp.bfloat16)
        roll_ref[1:, span((2 * zi + x) * rows + quarters[n] * sub, sub), :] = stage_out[n, head]

    def send_masters(n, which):
        for e in which:
            put(stage_out.at[n, near[e] % KV_HEADS], block(zi, x, halves_at[n]), (r, near[e] * 2 + x),
                MASTERS, m1[n][e - 1])

    stage_masters(0)
    send_masters(0, range(1, z_count))
    spread_in = [numbered() for _ in range(z_count)]

    def second_block(e, device):
        here = block(near[e], x, 1 - yi)
        put(here, here, device, FORWARD, FORWARD)

    def spread_block(e):
        if e:
            with jax.named_scope(f'w_m1#{e}'):
                master_in(0, e).wait_recv()
        here = block(near[e], x, yi)
        put(here, here, beside, SPREAD, spread_in[e])
        put(here, here, mate, TO_MATE, TO_MATE)

    def forward_block(e, up):
        got = block(near[e], 1 - x, yi)
        with jax.named_scope(f'w_sp#{e}'):
            landing(got, spread_in[e]).wait_recv()
        if up:
            put(got, got, above, FORWARD, FORWARD)
        put(got, got, mate, TO_MATE, TO_MATE)

    spread_block(0)

    for copy in fetch_tokens:
        copy.wait()
    terms = token_rows(ids_in[0:1], ids_in[1:2], logp_in[0:1], logp_in[1:2], logp_in[2:3])
    for j, row in enumerate(terms):
        token_own[j:j + 1, :toks] = row
    mate_tok.start()
    if both == 2:
        stage_masters(1)
        second_block(0, beside)

    is_home = home_z == zi
    fetch_m0.wait()

    @pl.when(is_home)
    def _():
        at = span(home_piece * final, final)
        for h in range(KV_HEADS):
            low = KV_HEADS * HEAD + h * HEAD
            base_out[h, :, :HEAD] = m0[at, h * HEAD:(h + 1) * HEAD].astype(jnp.bfloat16)
            base_out[h, :, HEAD:] = m0[at, low:low + HEAD].astype(jnp.bfloat16)
        for d in range(1, z_count):
            put(base_out.at[(head + d) % KV_HEADS], base_in, z_peers[d], BASE, BASE)
        base_in[...] = base_out[head]

    with jax.named_scope('w_hid'):
        fetch_hid.wait()
        mate_hid.wait_recv()

    @pl.loop(0, half // WIDE)
    def _(t):
        at = pl.multiple_of(t * WIDE, WIDE)
        hid_t[pl.ds(at, WIDE), :] = jnp.transpose(hid[:, pl.ds(at, WIDE)])

    with jax.named_scope('w_cot'):
     fetch_cot.wait()
    mate_cot.wait_recv()
    mate_info.wait_recv()
    mate_tok.wait_recv()
    with jax.named_scope('w_stats'):
        stats.wait_recv()
    total = own_sums + jnp.sum(stat_in[...], axis=0)
    wide = shape[1]
    count = jnp.maximum(total, 1.0)
    mean = pltpu.roll(total, wide - groups, 1) / count
    spread_of = jnp.maximum(
        jnp.sqrt(jnp.maximum(pltpu.roll(total, wide - 2 * groups, 1) / count - mean * mean, 0.0)), 0.5)

    def coef_of(told, token):
        hots, given = told[:SEQ_DEV], told[SEQ_DEV:, 0:1]
        advantage = (given - jnp.sum(hots * mean, axis=1, keepdims=True)) / jnp.sum(
            hots * spread_of, axis=1, keepdims=True)
        out = token[SEQ_DEV:SEQ_DEV + 1]
        for j in range(SEQ_DEV):
            out = out + token[j:j + 1] * advantage[j:j + 1]
        return jnp.transpose(jnp.broadcast_to(out, (LANES, out.shape[1])))[:toks]

    coefs = [coef_of(info, token_own[...]), coef_of(info_in[...], token_in[...])]

    lens, offsets = [half], [0]
    for i in range(dims):
        lens.append(lens[-1] // 2)
        offsets.append(offsets[-1] + bits[i] * lens[-1])
    starts, at = [], 0
    for length in lens[1:]:
        starts.append(at)
        at += length
    turns = [2, 1, 3, 0]
    order = [(head + d) % KV_HEADS for d in turns]
    tile = half // 2
    chunks = 2 * KV_HEADS
    inbound = {(i, k): numbered() for i in range(dims) for k in range(chunks)}

    def halves(i, k):
        gone = offsets[i] + (1 - bits[i]) * lens[i + 1]
        return pltpu.make_async_remote_copy(
            src_ref=part.at[order[k // 2], k % 2, span(gone, lens[i + 1])],
            dst_ref=sums.at[order[k // 2], k % 2, pl.ds(starts[i], lens[i + 1])],
            send_sem=set_send.at[HALVES], recv_sem=set_recv.at[inbound[i, k]],
            device_id=partners[i], device_id_type=MESH)

    def pass_on(i, k):
        halves(i, k).start()

    for k in range(KV_HEADS):
        h = order[k]
        for side in range(2):
            low = pl.ds(pl.multiple_of(side * KV_HEADS * HEAD + h * HEAD, HEAD), HEAD)
            for src in range(2):
                delta[src * toks:(src + 1) * toks, side * HEAD:(side + 1) * HEAD] = (
                    coefs[src] * cot[src, :, low].astype(jnp.float32)).astype(jnp.bfloat16)
        for t in range(2):
          with jax.named_scope(f'mul#k={k}'):
            out = jnp.dot(
                hid_t[t * tile:(t + 1) * tile, :], delta[...], preferred_element_type=jnp.float32
            ).astype(jnp.bfloat16)
            for q in range(tile // final):
                j = t * (tile // final) + q
                place = spot(j, 0) + core * (spot(j, 1) - spot(j, 0))
                for side in range(2):
                    part[h, side, span(place * final, final), :] = (
                        out[q * final:(q + 1) * final, side * HEAD:(side + 1) * HEAD])
        pass_on(0, 2 * k)
        pass_on(0, 2 * k + 1)
        if k == 0:
            spread_block(1)
    if both == 2:
        send_masters(1, [e for e in range(1, z_count) if e != 2])

    inner = min(final, 112)

    def add_in(i, k):
        h, side = order[k // 2], k % 2

        @pl.loop(0, lens[i + 1] // inner)
        def _(t):
            at = span(offsets[i + 1] + t * inner, inner)
            part[h, side, at, :] = (
                part[h, side, at, :].astype(jnp.float32)
                + sums[h, side, span(starts[i] + t * inner, inner), :].astype(jnp.float32)
            ).astype(jnp.bfloat16)

    last = dims - 1
    mine = span(offsets[dims], final)
    z_in = {(d, side): numbered() for side in range(2) for d in range(1, z_count)}

    def z_copy(d, side):
        return pltpu.make_async_remote_copy(
            src_ref=part.at[(head + d) % KV_HEADS, side, mine], dst_ref=zin.at[d - 1, side],
            send_sem=set_send.at[GRADS], recv_sem=set_recv.at[z_in[d, side]],
            device_id=z_peers[d], device_id_type=MESH)

    def z_send(k):
        for d in range(1, z_count):
            if d % KV_HEADS == turns[k // 2]:
                z_copy(d, k % 2).start()

    far = z_count > KV_HEADS
    for t in range(chunks + last):
        for i in range(dims):
            k = t - i
            if k < 0 or k >= chunks:
                continue
            with jax.named_scope(f'w_in#i={i}#k={k}'):
                halves(i, k).wait_recv()
            if i == last and k // 2 == KV_HEADS - 1 and not far:
                side = k % 2
                grad[:, side * HEAD:(side + 1) * HEAD] = (
                    part[head, side, mine, :].astype(jnp.float32)
                    + sums[head, side, pl.ds(starts[last], final), :].astype(jnp.float32))
                continue
            add_in(i, k)
            if i < last:
                pass_on(i + 1, k)
            else:
                z_send(k)
        if t == 5:
            forward_block(0, False)
            forward_block(1, both == 2)
        if t == chunks - 2 and both == 2 and z_count > 2:
            send_masters(1, [2])
    if far:
        for side in range(2):
            grad[:, side * HEAD:(side + 1) * HEAD] = part[head, side, mine, :].astype(jnp.float32)

    arrivals = [d for turn in turns for d in range(1, z_count) if d % KV_HEADS == turn]
    own_square = jnp.zeros((1, HEAD), jnp.float32)
    for d in arrivals:
        for side in range(2):
            with jax.named_scope(f'w_z#{d}'):
                z_copy(d, side).wait_recv()
            cut = slice(side * HEAD, (side + 1) * HEAD)
            g = grad[:, cut] + zin[d - 1, side].astype(jnp.float32)
            grad[:, cut] = g
            if d == arrivals[-1]:
                own_square = own_square + jnp.sum(g * g, axis=0, keepdims=True)
                grad_b[:, cut] = g.astype(jnp.bfloat16)

    own_square = jnp.broadcast_to(jnp.sum(own_square, axis=1, keepdims=True), (1, LANES))
    small[1, :, :LANES] = own_square
    all_squares = to_all(small.at[1, :, pl.ds(0, LANES)], square_in, 2)

    relayed = n_rep == 4 and pieces == 1
    relay_at = [numbered(), numbered()]
    y_other = flip(y, 0)[0] if relayed else y
    other_z = home(y_other)[0]
    nm_in = [numbered() for _ in range(KV_HEADS * pieces)][0]
    here_rows = rows_in.at[head, span(home_piece * final, final)]
    if relayed:
        for u in range(2):
            cut = pl.ds(u * (final // 2), final // 2)
            put(grad_b.at[cut], relay_in.at[cut], above, RELAY, relay_at[u])
        nm_copies = [
            (home_z != zi, copy_to(grad_b, here_rows, (r, 2 * home_z + x), RETURN, nm_in + head)),
            (other_z != zi, copy_to(relay_in, here_rows, (r, 2 * other_z + x), RETURN + 1, nm_in + head))]
        relay_out = [
            copy_to(relay_in.at[pl.ds(u * (final // 2), final // 2)],
                    rows_in.at[head, pl.ds(u * (final // 2), final // 2)],
                    (r, 2 * other_z + x), RETURN + 1, nm_in + head)
            for u in range(2)]
        pl.when(home_z != zi)(nm_copies[0][1].start)
    else:
        nm_copies = []
        for j in range(n_rep // 2):
            copy = copy_to(
                grad_b, here_rows, (2 * j + core, 2 * home_z + x),
                RETURN + j, nm_in + head * pieces + home_piece)
            leaves = (home_z // KV_HEADS == zi // KV_HEADS) & ((home_z != zi) | (j != y))
            nm_copies.append((leaves, copy))
            pl.when(leaves)(copy.start)

    @pl.when(is_home)
    def _():
        rows_in[head, span(home_piece * final, final), :] = grad_b[...]

    for e in range(2, z_count):
        spread_block(e)
    if both == 2:
        for e in range(3, z_count):
            master_in(1, e).wait_recv()
            second_block(e, beside)

    @pl.when(home_z != zi)
    def _():
        whole(base_in, BASE).wait_recv()

    with jax.named_scope('w_squares'):
        all_squares.wait_recv()
    square = own_square + jnp.sum(square_in[...], axis=0)
    rms = jnp.sqrt(square[:, 0:1] / (features * KV_HEADS * WIDE) + 1e-06)
    scale = 0.5 / rms
    row_me = row_of(y, x)

    @pl.loop(0, final // inner)
    def _(t):
        at = span(t * inner, inner)
        roll_ref[0, span(row_me + t * inner, inner), :] = (
            base_in[at, :].astype(jnp.float32) - scale * grad[at, :]).astype(jnp.bfloat16)

    parts = 2 if final // 2 % SUB == 0 else 1
    size = final // parts
    level_in = [[numbered() for _ in range(parts)] for _ in range(dims)]

    def layer0(yy, xx, u):
        return roll_ref.at[0, span(row_of(yy, xx) + u * size, size), :]

    def gather_in(i, u):
        return landing(roll_ref.at[0, pl.ds(0, size << (dims - 1 - i)), :], level_in[i][u])

    def gather_out(i, u):
        for at in have[:1 << (last - i)]:
            here = layer0(*at, u)
            put(here, here, partners[i], GATHER, level_in[i][u])

    def piece_out(at):
        for u in range(parts):
            here = layer0(*at, u)
            put(here, here, mate, PIECES, PIECES)

    have = [(y, x)]
    for i in reversed(range(dims)):
        have = have + [across(*at, i) for at in have]
    for u in range(parts):
        gather_out(last, u)
    piece_out(have[0])
    if relayed:
        for u in range(2):
            with jax.named_scope('w_relay'):
                landing(relay_in.at[pl.ds(u * (final // 2), final // 2)], relay_at[u]).wait_recv()
            pl.when(other_z != zi)(relay_out[u].start)

        @pl.when(other_z == zi)
        def _():
            rows_in[head] = relay_in[...]
    if z_count > 2:
        forward_block(2, both == 2)
    for i in reversed(range(last)):
        for u in range(parts):
            with jax.named_scope(f'w_ag#{i + 1}#{u}'):
                gather_in(i + 1, u).wait_recv()
            gather_out(i, u)
        for at in have[1 << (last - 1 - i):1 << (last - i)]:
            piece_out(at)

    keeper = zi // half_z
    hand_in = [numbered() for _ in range(KV_HEADS)]
    hand_over = [copy_to(rows_in.at[h], rows_in.at[h], mate, HAND, hand_in[h]) for h in range(KV_HEADS)]

    def landed(h, p):
        return landing(rows_in.at[h, pl.ds(p * final, final)], nm_in + h * pieces + p)

    @pl.when(core == keeper)
    @jax.named_scope('w_rows')
    def _():
        low = zi + core * (z_count - 1 - 2 * zi)
        for h in range(KV_HEADS):
            for p in range(pieces):
                @pl.when((h != head) if relayed else (h != head) | (y != low * pieces + p))
                def _():
                    landed(h, p).wait_recv()
            hand_over[h].start()

    blocks = roll_ref.at[pl.ds(1, layer_count - 1), pl.ds(0, z_count * sub), :]
    for e in range(3, z_count):
        forward_block(e, False)
    if both == 2:
        for e in range(1, min(z_count, 3)):
            with jax.named_scope(f'w_m2#{e}'):
                master_in(1, e).wait_recv()
        with jax.named_scope('w_fwd'):
            whole(blocks, FORWARD).wait_recv()
        for z in near:
            for xx in (x, 1 - x):
                got = block(z, xx, 1 - yi)
                put(got, got, mate, TO_MATE, TO_MATE)
    with jax.named_scope('w_gathered'):
        for u in range(parts):
            gather_in(0, u).wait_recv()
            for at in have[n_rep // 2:]:
                here = layer0(*at, u)
                put(here, here, mate, PIECES, PIECES)

    @pl.when(core != keeper)
    @jax.named_scope('w_hand')
    def _():
        for copy in hand_over:
            copy.wait_recv()

    for h in range(KV_HEADS):
        for side in range(2):
            low = side * KV_HEADS * HEAD + h * HEAD
            nm_ref[:, low:low + HEAD] = (
                m0[:, low:low + HEAD] - scale * rows_in[h, :, side * HEAD:(side + 1) * HEAD].astype(jnp.float32))

    all_blocks = roll_ref.at[pl.ds(1, layer_count - 1), pl.ds(0, z_count * split * sub), :]
    all_pieces = roll_ref.at[0, pl.ds(0, n_rep * final), :]
    with jax.named_scope('w_mate'):
        whole(all_blocks, TO_MATE).wait_recv()
        whole(all_pieces, PIECES).wait_recv()

    @pl.when(core == keeper)
    def _():
        whole(rows_in, HAND).wait_send()

    @pl.when(is_home)
    def _():
        whole(zin, BASE).wait_send()

    for leaves, copy in nm_copies:
        pl.when(leaves)(copy.wait_send)
    for copy in mate_copies:
        copy.wait_send()
    whole(roll_ref.at[pl.ds(1, layer_count - 1), pl.ds(0, (z_count - 1) * both * sub), :], MASTERS).wait_send()
    whole(blocks, SPREAD).wait_send()
    if both == 2:
        whole(blocks, FORWARD).wait_send()
    if relayed:
        whole(relay_in, RELAY).wait_send()
    whole(all_blocks, TO_MATE).wait_send()
    whole(all_pieces, PIECES).wait_send()
    whole(roll_ref.at[0, pl.ds(0, (n_rep - 1) * final), :], GATHER).wait_send()
    whole(part.at[:, :, pl.ds(0, half - final), :], HALVES).wait_send()
    whole(zin, GRADS).wait_send()
    stats.wait_send()
    all_squares.wait_send()


def per_device(
    n_rep, n_shard, hidden, cotangent, seq_ids, response_mask, group_ids, rewards, new_logp, old_logp, ref_logp,
    master,
):
    everyone = n_rep * n_shard
    groups = everyone * SEQ_DEV // 8
    wide = -(-3 * groups // LANES) * LANES
    toks, features = hidden.shape
    layer_count, rows, cols = master.shape
    z_count = n_shard // 2
    split = 4 if n_rep % 4 == 0 and (rows // 4) % SUB == 0 else 2
    sub = rows // split
    half = features // 2
    final = half // n_rep
    pad = -(-toks // LANES) * LANES
    bf16, f32 = jnp.bfloat16, jnp.float32
    vmem, hbm = pl.BlockSpec(memory_space=pltpu.VMEM), pl.BlockSpec(memory_space=pltpu.HBM)
    dims = n_rep.bit_length() - 1
    both = 2 if split == 4 else 1
    landings = 7 + 4 + 2 + KV_HEADS + both * (z_count - 1) + z_count + 8 * dims + 2 * (z_count - 1) + KV_HEADS * (n_rep // z_count) + 2 * dims
    return pl.pallas_call(
        functools.partial(step_kernel, n_rep, n_shard, split, groups),
        out_shape=(pltpu.VMEM((rows, cols), f32), pltpu.VMEM((layer_count, features, WIDE), bf16)),
        in_specs=[hbm] * 10,
        out_specs=(vmem, vmem),
        scratch_shapes=[
            pltpu.SMEM((1, SEQ_DEV), jnp.int32),
            pltpu.SMEM((1, SEQ_DEV), f32),
            pltpu.VMEM((2, toks), jnp.int32),
            pltpu.VMEM((3, toks), f32),
            pltpu.VMEM((2, 1, wide), f32),
            pltpu.VMEM((everyone - 1, 1, wide), f32),
            pltpu.VMEM((everyone - 1, 1, LANES), f32),
            pltpu.VMEM((8, wide), f32),
            pltpu.VMEM((8, wide), f32),
            pltpu.VMEM((8, pad), f32),
            pltpu.VMEM((8, pad), f32),
            pltpu.VMEM((2 * toks, half), bf16),
            pltpu.VMEM((half, 2 * toks), bf16),
            pltpu.VMEM((2, toks, cols), bf16),
            pltpu.VMEM((2 * toks, WIDE), bf16),
            pltpu.VMEM((KV_HEADS, 2, half, HEAD), bf16),
            pltpu.VMEM((KV_HEADS, 2, half, HEAD), bf16),
            pltpu.VMEM((z_count - 1, 2, final, HEAD), bf16),
            pltpu.VMEM((final, WIDE), f32),
            pltpu.VMEM((final, WIDE), bf16),
            pltpu.VMEM((final, WIDE), bf16),
            pltpu.VMEM((KV_HEADS, final, WIDE), bf16),
            pltpu.VMEM((final, WIDE), bf16),
            pltpu.VMEM((rows, cols), f32),
            pltpu.VMEM((2, layer_count - 1, sub, cols), f32),
            pltpu.VMEM((2, KV_HEADS, layer_count - 1, sub, WIDE), bf16),
            pltpu.VMEM((KV_HEADS, rows, WIDE), bf16),
            pltpu.SemaphoreType.DMA((12,)),
            pltpu.SemaphoreType.DMA((4,)),
            pltpu.SemaphoreType.DMA((16 + n_rep // 2,)),
            pltpu.SemaphoreType.DMA((landings,)),
        ],
        compiler_params=pltpu.CompilerParams(
            collective_id=0, has_side_effects=True, vmem_limit_bytes=44 * 2**20
        ),
        name="step",
    )(*(pltpu.with_memory_space_constraint(value, pltpu.HBM) for value in (
        group_ids, rewards, seq_ids, response_mask, new_logp, old_logp, ref_logp, hidden, cotangent, master)))


def solution(mesh):
    tokens = P(("rep", "shard"), None)
    return jax.shard_map(
        functools.partial(per_device, mesh.shape["rep"], mesh.shape["shard"]),
        mesh=mesh,
        in_specs=(tokens,) * 9 + (P(None, "shard", None),),
        out_specs=(P("shard", None), P(None, None, "shard")),
        check_vma=False,
    )
```

```python
import functools

import jax
import jax.numpy as jnp
from jax import lax
from jax.experimental import pallas as pl
from jax.experimental.pallas import tpu as pltpu
from jax.sharding import PartitionSpec as P

HEAD = 128
KV_HEADS = 4
SEQ_DEV = 4
WIDE = 2 * HEAD
LANES = 128
SUB = 16
MESH = pl.DeviceIdType.MESH


def token_rows(seq_row, mask_row, new_row, old_row, ref_row):
    maskf = mask_row.astype(jnp.float32)
    onehot = [(seq_row == j).astype(jnp.float32) for j in range(SEQ_DEV)]
    tok_len = jnp.zeros_like(maskf)
    for hot in onehot:
        tok_len = tok_len + hot * jnp.maximum(jnp.sum(maskf * hot, axis=1, keepdims=True), 1.0)
    weight = maskf / tok_len
    ratio = -weight * jnp.exp(new_row - old_row)
    return [hot * ratio for hot in onehot] + [weight * (0.2 * (1.0 - jnp.exp(ref_row - new_row)))]


def flip(index, bit):
    step = 1 << bit
    here = (index // step) % 2
    return index + (1 - 2 * here) * step, here


def step_kernel(
    n_rep, n_shard, split, groups, group_hbm, reward_hbm, *args,
):
    token_hbm, args = args[:5], args[5:]
    step_body(n_rep, n_shard, split, groups, group_hbm, reward_hbm, token_hbm, *args)


def step_body(
    n_rep, n_shard, split, groups, group_hbm, reward_hbm, token_hbm,
    hidden_ref, cot_ref, master_ref,
    nm_ref, roll_ref,
    group_ref, reward_ref, ids_in, logp_in, small, stat_in, square_in, info_in, info_own, token_own, token_in, hid, hid_t, cot, delta, part, sums, zin,
    grad, grad_b, relay_in, base_out, base_in, m0, stage_in, stage_out, rows_in,
    local_sems, all_sems, set_send, set_recv,
):
    z_count = n_shard // 2
    dims = n_rep.bit_length() - 1
    everyone = n_rep * n_shard
    r, s = lax.axis_index("rep"), lax.axis_index("shard")
    me = r * n_shard + s
    core, y, x, zi = r % 2, r // 2, s % 2, s // 2
    head = zi % KV_HEADS
    toks, features = hidden_ref.shape
    half = features // 2
    layer_count, rows, cols = master_ref.shape
    sub = rows // split
    final = half // n_rep
    pieces = rows // final
    half_z = z_count // 2
    counter = [0]
    (SPREAD, FORWARD, TO_MATE, PIECES, BASE, RELAY, HAND,
     MASTERS, GATHER, HALVES, GRADS, RETURN) = range(12)
    given_in, given_out = 7, 12
    mate = (flip(r, 0)[0], s)

    def numbered():
        number = given_in + counter[0]
        counter[0] += 1
        return number

    def copy_to(src, dst, device, gone, landed):
        return pltpu.make_async_remote_copy(
            src_ref=src, dst_ref=dst, send_sem=set_send.at[gone], recv_sem=set_recv.at[landed],
            device_id=device, device_id_type=MESH)

    def put(src, dst, device, gone, landed):
        copy_to(src, dst, device, gone, landed).start()

    def whole(ref, number):
        return copy_to(ref, ref, mate, number, number)

    def landing(ref, number):
        return copy_to(ref, ref, mate, 0, number)

    def local(src, dst, number):
        copy = pltpu.make_async_copy(src, dst, local_sems.at[number])
        copy.start()
        return copy

    def span(at, size):
        return pl.ds(pl.multiple_of(at, SUB), size)

    def to_all(src, dst, sem):
        @pl.loop(1, everyone)
        def _(i):
            peer = (me + i) % everyone
            pltpu.make_async_remote_copy(
                src_ref=src, dst_ref=dst.at[i - 1], send_sem=all_sems.at[sem], recv_sem=all_sems.at[sem + 1],
                device_id=(peer // n_shard, peer % n_shard), device_id_type=MESH).start()

        return pltpu.make_async_remote_copy(
            src_ref=dst, dst_ref=dst, send_sem=all_sems.at[sem], recv_sem=all_sems.at[sem + 1],
            device_id=(flip(r, 0)[0], s), device_id_type=MESH)

    options = []
    for bit in range(1, dims):
        other, here = flip(r, bit)
        options.append((other, s, here))
    other, here = flip(s, 0)
    options.append((r, other, here))
    partners, bits = [], []
    for i in range(dims):
        a, b = options[i], options[(i + 1) % dims]
        partners.append(tuple(a[k] + core * (b[k] - a[k]) for k in range(2)))
        bits.append(a[2] + core * (b[2] - a[2]))
    z_peers = [None] + [(r, ((zi + d) % z_count) * 2 + x) for d in range(1, z_count)]

    def home(yy):
        low = yy // pieces
        return low + core * (z_count - 1 - 2 * low), yy % pieces

    def row_of(yy, xx):
        z, piece = home(yy)
        return (2 * z + xx) * rows + piece * final

    def across(yy, xx, i):
        moved = []
        for option in (i % dims, (i + 1) % dims):
            moved.append((flip(yy, option)[0], xx) if option < dims - 1 else (yy, 1 - xx))
        (ya, xa), (yb, xb) = moved
        return ya + core * (yb - ya), xa + core * (xb - xa)

    def spot(j, c):
        low, xx, piece = j // pieces // 2, j // pieces % 2, j % pieces
        yy = (low if c == 0 else half_z - 1 - low) * pieces + piece
        chosen = [(yy >> o) & 1 for o in range(dims - 1)] + [xx]
        return sum(chosen[(i + c) % dims] << (dims - 1 - i) for i in range(dims))

    home_z, home_piece = home(y)
    quarter = r % split
    own_half = pl.ds(pl.multiple_of(core * half, LANES), half)
    other_half = pl.ds(pl.multiple_of((1 - core) * half, LANES), half)
    yi = quarter // 2
    both = 2 if split == 4 else 1
    quarters = [quarter, quarter + (1 - 2 * yi) * 2][:both]
    fetch_stage = [
        local(master_ref.at[pl.ds(1, layer_count - 1), span(q * sub, sub), :], stage_in.at[n], (0, 11)[n])
        for n, q in enumerate(quarters)]
    fetch_hid = local(hidden_ref.at[:, own_half], hid.at[pl.ds(0, toks)], 1)
    fetch_cot = local(cot_ref, cot.at[0], 2)
    fetch_m0 = local(master_ref.at[0], m0, 3)
    fetch_small = [local(group_hbm, group_ref, 4), local(reward_hbm, reward_ref, 5)]
    fetch_tokens = [local(ref, ids_in.at[pl.ds(n, 1)], 6 + n) for n, ref in enumerate(token_hbm[:2])]
    fetch_tokens += [local(ref, logp_in.at[pl.ds(n, 1)], 8 + n) for n, ref in enumerate(token_hbm[2:])]

    barrier = pltpu.get_barrier_semaphore()

    @pl.loop(1, everyone)
    def _(i):
        peer = (me + i) % everyone
        pl.semaphore_signal(
            barrier, inc=1, device_id=(peer // n_shard, peer % n_shard), device_id_type=MESH)

    shape = info_in.shape
    line = lax.broadcasted_iota(jnp.int32, shape, 0)
    lane = lax.broadcasted_iota(jnp.int32, shape, 1)
    row_lane = lax.broadcasted_iota(jnp.int32, (1, shape[1]), 1)
    info = jnp.zeros(shape, jnp.float32)
    own_sums = jnp.zeros((1, shape[1]), jnp.float32)
    for copy in fetch_small:
        copy.wait()
    for j in range(SEQ_DEV):
        group, given = group_ref[0, j], reward_ref[0, j]
        info = jnp.where((line == j) & (lane == group), 1.0, info)
        info = jnp.where(line == SEQ_DEV + j, given, info)
        for n, value in enumerate((1.0, given, given * given)):
            own_sums = own_sums + jnp.where(row_lane == n * groups + group, value, 0.0)
    info_own[...] = info
    small[0] = own_sums
    token_own[...] = jnp.zeros_like(token_own)
    with jax.named_scope('w_barrier'):
        pl.semaphore_wait(barrier, everyone - 1)

    stats = to_all(small.at[0], stat_in, 0)
    sent_out = n_rep // 2 + given_out
    mate_copies = [
        copy_to(src, dst, mate, sent_out + n, numbered()) for n, (src, dst) in enumerate((
            (info_own, info_in), (hidden_ref.at[:, other_half], hid.at[pl.ds(toks, toks)]), (cot_ref, cot.at[1]),
            (token_own, token_in)))]
    mate_info, mate_hid, mate_cot, mate_tok = mate_copies
    for copy in mate_copies[:3]:
        copy.start()

    def block(z, xx, yy):
        return roll_ref.at[pl.ds(1, layer_count - 1), span((2 * z + xx) * rows + (2 * yy + core) * sub, sub), :]

    near = [zi]
    for e in range(1, z_count):
        z = zi
        for bit in range(z_count.bit_length() - 1):
            if e >> bit & 1:
                z = flip(z, bit)[0]
        near.append(z)
    beside = (r, flip(s, 0)[0])
    above = (flip(r, 1)[0], s)
    halves_at = [yi, 1 - yi]
    m1 = [[numbered() for _ in range(1, z_count)] for _ in range(both)]

    def master_in(n, e):
        return landing(block(zi, x, halves_at[n]), m1[n][e - 1])

    def stage_masters(n):
        with jax.named_scope('w_stage'):
            fetch_stage[n].wait()
        for h in range(KV_HEADS):
            low = KV_HEADS * HEAD + h * HEAD
            for l in range(layer_count - 1):
                stage_out[n, h, l, :, :HEAD] = stage_in[n, l, :, h * HEAD:(h + 1) * HEAD].astype(jnp.bfloat16)
                stage_out[n, h, l, :, HEAD:] = stage_in[n, l, :, low:low + HEAD].astype(jnp.bfloat16)
        roll_ref[1:, span((2 * zi + x) * rows + quarters[n] * sub, sub), :] = stage_out[n, head]

    def send_masters(n, which):
        for e in which:
            put(stage_out.at[n, near[e] % KV_HEADS], block(zi, x, halves_at[n]), (r, near[e] * 2 + x),
                MASTERS, m1[n][e - 1])

    stage_masters(0)
    send_masters(0, range(1, z_count))
    spread_in = [numbered() for _ in range(z_count)]

    def second_block(e, device):
        here = block(near[e], x, 1 - yi)
        put(here, here, device, FORWARD, FORWARD)

    def spread_block(e):
        if e:
            with jax.named_scope(f'w_m1#{e}'):
                master_in(0, e).wait_recv()
        here = block(near[e], x, yi)
        put(here, here, beside, SPREAD, spread_in[e])
        put(here, here, mate, TO_MATE, TO_MATE)

    def forward_block(e, up):
        got = block(near[e], 1 - x, yi)
        with jax.named_scope(f'w_sp#{e}'):
            landing(got, spread_in[e]).wait_recv()
        if up:
            @pl.when(core == 0)
            def _():
                put(got, got, above, FORWARD, FORWARD)
        put(got, got, mate, TO_MATE, TO_MATE)

    spread_block(0)

    for copy in fetch_tokens:
        copy.wait()
    terms = token_rows(ids_in[0:1], ids_in[1:2], logp_in[0:1], logp_in[1:2], logp_in[2:3])
    for j, row in enumerate(terms):
        token_own[j:j + 1, :toks] = row
    mate_tok.start()
    if both == 2:
        stage_masters(1)
        second_block(0, beside)

    is_home = home_z == zi
    fetch_m0.wait()

    @pl.when(is_home)
    def _():
        at = span(home_piece * final, final)
        for h in range(KV_HEADS):
            low = KV_HEADS * HEAD + h * HEAD
            base_out[h, :, :HEAD] = m0[at, h * HEAD:(h + 1) * HEAD].astype(jnp.bfloat16)
            base_out[h, :, HEAD:] = m0[at, low:low + HEAD].astype(jnp.bfloat16)
        for d in range(1, z_count):
            put(base_out.at[(head + d) % KV_HEADS], base_in, z_peers[d], BASE, BASE)
        base_in[...] = base_out[head]

    with jax.named_scope('w_hid'):
        fetch_hid.wait()
        mate_hid.wait_recv()

    @pl.loop(0, half // WIDE)
    def _(t):
        at = pl.multiple_of(t * WIDE, WIDE)
        hid_t[pl.ds(at, WIDE), :] = jnp.transpose(hid[:, pl.ds(at, WIDE)])

    with jax.named_scope('w_cot'):
     fetch_cot.wait()
    mate_cot.wait_recv()
    mate_info.wait_recv()
    mate_tok.wait_recv()
    with jax.named_scope('w_stats'):
        stats.wait_recv()
    total = own_sums + jnp.sum(stat_in[...], axis=0)
    wide = shape[1]
    count = jnp.maximum(total, 1.0)
    mean = pltpu.roll(total, wide - groups, 1) / count
    spread_of = jnp.maximum(
        jnp.sqrt(jnp.maximum(pltpu.roll(total, wide - 2 * groups, 1) / count - mean * mean, 0.0)), 0.5)

    def coef_of(told, token):
        hots, given = told[:SEQ_DEV], told[SEQ_DEV:, 0:1]
        advantage = (given - jnp.sum(hots * mean, axis=1, keepdims=True)) / jnp.sum(
            hots * spread_of, axis=1, keepdims=True)
        out = token[SEQ_DEV:SEQ_DEV + 1]
        for j in range(SEQ_DEV):
            out = out + token[j:j + 1] * advantage[j:j + 1]
        return jnp.transpose(jnp.broadcast_to(out, (LANES, out.shape[1])))[:toks]

    coefs = [coef_of(info, token_own[...]), coef_of(info_in[...], token_in[...])]

    lens, offsets = [half], [0]
    for i in range(dims):
        lens.append(lens[-1] // 2)
        offsets.append(offsets[-1] + bits[i] * lens[-1])
    starts, at = [], 0
    for length in lens[1:]:
        starts.append(at)
        at += length
    turns = [2, 1, 3, 0]
    order = [(head + d) % KV_HEADS for d in turns]
    paired = z_count == KV_HEADS
    pair_z = flip(zi, 0)[0]
    inner_plane = (zi + 1) // 2 % 2 == 1
    if paired:
        outer_z = (1 - zi // 2) * 3
        order = [outer_z, flip(outer_z, 0)[0], pair_z, zi]
    tile = half // 2
    chunks = 2 * KV_HEADS
    inbound = {(i, k): numbered() for i in range(dims) for k in range(chunks)}

    def halves(i, k):
        gone = offsets[i] + (1 - bits[i]) * lens[i + 1]
        return pltpu.make_async_remote_copy(
            src_ref=part.at[order[k // 2], k % 2, span(gone, lens[i + 1])],
            dst_ref=sums.at[order[k // 2], k % 2, pl.ds(starts[i], lens[i + 1])],
            send_sem=set_send.at[HALVES], recv_sem=set_recv.at[inbound[i, k]],
            device_id=partners[i], device_id_type=MESH)

    def pass_on(i, k):
        halves(i, k).start()

    def multiply_at(h, top, n):
        where = [[[spot(j, c) for j in range(n_rep)].index(b * (n_rep // 2) + n) for b in range(2)] for c in range(2)]
        (a, b), (a1, b1) = where
        low, high = a + core * (a1 - a), b + core * (b1 - b)
        out = jnp.dot(
            hid_t[span((low + top * (high - low)) * final, final), :], delta[...], preferred_element_type=jnp.float32
        ).astype(jnp.bfloat16)
        at = span((top * (n_rep // 2) + n) * final, final)
        for side in range(2):
            part[h, side, at, :] = out[:, side * HEAD:(side + 1) * HEAD]

    for k in range(KV_HEADS):
        h = order[k]
        for side in range(2):
            low = pl.ds(pl.multiple_of(side * KV_HEADS * HEAD + h * HEAD, HEAD), HEAD)
            for src in range(2):
                delta[src * toks:(src + 1) * toks, side * HEAD:(side + 1) * HEAD] = (
                    coefs[src] * cot[src, :, low].astype(jnp.float32)).astype(jnp.bfloat16)
        if k == 0:
            for stays in (0, 1):
                for n in range(n_rep // 2):
                    multiply_at(h, bits[0] if stays else 1 - bits[0], n)
                if not stays:
                    pass_on(0, 0)
                    pass_on(0, 1)
            continue
        for t in range(2):
          with jax.named_scope(f'mul#k={k}'):
            out = jnp.dot(
                hid_t[t * tile:(t + 1) * tile, :], delta[...], preferred_element_type=jnp.float32
            ).astype(jnp.bfloat16)
            for q in range(tile // final):
                j = t * (tile // final) + q
                place = spot(j, 0) + core * (spot(j, 1) - spot(j, 0))
                for side in range(2):
                    part[h, side, span(place * final, final), :] = (
                        out[q * final:(q + 1) * final, side * HEAD:(side + 1) * HEAD])
        pass_on(0, 2 * k)
        pass_on(0, 2 * k + 1)
    spread_block(1)
    if both == 2:
        send_masters(1, [e for e in range(1, z_count) if e != 2])

    inner = min(final, 112)

    def add_in(i, k):
        h, side = order[k // 2], k % 2

        @pl.loop(0, lens[i + 1] // inner)
        def _(t):
            at = span(offsets[i + 1] + t * inner, inner)
            part[h, side, at, :] = (
                part[h, side, at, :].astype(jnp.float32)
                + sums[h, side, span(starts[i] + t * inner, inner), :].astype(jnp.float32)
            ).astype(jnp.bfloat16)

    last = dims - 1
    mine = span(offsets[dims], final)
    sources = range(2) if paired else range(z_count - 1)
    z_in = {(n, side): numbered() for side in range(2) for n in sources}
    z_mid = [numbered() for _ in range(4)] if paired else []

    def z_put(k, landing_ref, number, z):
        put(part.at[order[k // 2], k % 2, mine], landing_ref, (r, 2 * z + x), GRADS, number)

    def z_send(k):
        if not paired:
            for d in range(1, z_count):
                if d % KV_HEADS == turns[k // 2]:
                    z_put(k, zin.at[d - 1, k % 2], z_in[d - 1, k % 2], (zi + d) % z_count)
        elif k < 4:
            @pl.when(jnp.logical_not(inner_plane))
            def _():
                z_put(k, zin.at[3 + k // 2, k % 2], z_mid[k], pair_z)
        elif k < 6:
            z_put(k, zin.at[1, k % 2], z_in[1, k % 2], pair_z)

    def z_combine(k):
        held = zin.at[3 + k // 2, k % 2]

        @pl.when(inner_plane)
        def _():
            with jax.named_scope(f'w_mid#{k}'):
                landing(held, z_mid[k]).wait_recv()
            h, side = order[k // 2], k % 2
            part[h, side, mine, :] = (
                part[h, side, mine, :].astype(jnp.float32) + held[...].astype(jnp.float32)).astype(jnp.bfloat16)
            z_put(k, zin.at[0, k % 2], z_in[0, k % 2], order[k // 2])

    far = z_count > KV_HEADS
    squares = {}

    def own_sum(side):
        for n in sources:
            with jax.named_scope(f'w_z#{n}'):
                landing(zin.at[n, side], z_in[n, side]).wait_recv()
        g = part[head, side, mine, :].astype(jnp.float32)
        if not far:
            g = g + sums[head, side, pl.ds(starts[last], final), :].astype(jnp.float32)
        for n in sources:
            g = g + zin[n, side].astype(jnp.float32)
        cut = slice(side * HEAD, (side + 1) * HEAD)
        grad[:, cut] = g
        grad_b[:, cut] = g.astype(jnp.bfloat16)
        squares[side] = jnp.sum(g * g, axis=0, keepdims=True)

    for t in range(chunks + last):
        for k in range(4 if paired else 0):
            if t == last + (3, 4, 5, 5)[k]:
                z_combine(k)
        for i in range(dims):
            k = t - i
            if k < 0 or k >= chunks:
                continue
            with jax.named_scope(f'w_in#i={i}#k={k}'):
                halves(i, k).wait_recv()
            if i == last and k // 2 == KV_HEADS - 1 and not far:
                own_sum(k % 2)
                continue
            add_in(i, k)
            if i < last:
                pass_on(i + 1, k)
            else:
                z_send(k)
        if both == 2 and t == 5 and z_count > 2:
            send_masters(1, [2])
        if t == 5:
            forward_block(0, False)
    if far:
        for side in range(2):
            own_sum(side)
    own_square = squares[0] + squares[1]
    own_square = jnp.broadcast_to(jnp.sum(own_square, axis=1, keepdims=True), (1, LANES))
    small[1, :, :LANES] = own_square
    all_squares = to_all(small.at[1, :, pl.ds(0, LANES)], square_in, 2)

    relayed = n_rep == 4 and pieces == 1
    relay_at = [numbered(), numbered()]
    y_other = flip(y, 0)[0] if relayed else y
    other_z = home(y_other)[0]
    nm_in = [numbered() for _ in range(KV_HEADS * pieces)][0]
    here_rows = rows_in.at[head, span(home_piece * final, final)]
    if relayed:
        for u in range(2):
            cut = pl.ds(u * (final // 2), final // 2)
            put(grad_b.at[cut], relay_in.at[cut], above, RELAY, relay_at[u])
        nm_copies = [
            (home_z != zi, copy_to(grad_b, here_rows, (r, 2 * home_z + x), RETURN, nm_in + head)),
            (other_z != zi, copy_to(relay_in, here_rows, (r, 2 * other_z + x), RETURN + 1, nm_in + head))]
        relay_out = [
            copy_to(relay_in.at[pl.ds(u * (final // 2), final // 2)],
                    rows_in.at[head, pl.ds(u * (final // 2), final // 2)],
                    (r, 2 * other_z + x), RETURN + 1, nm_in + head)
            for u in range(2)]
        pl.when(home_z != zi)(nm_copies[0][1].start)
    else:
        nm_copies = []
        for j in range(n_rep // 2):
            copy = copy_to(
                grad_b, here_rows, (2 * j + core, 2 * home_z + x),
                RETURN + j, nm_in + head * pieces + home_piece)
            leaves = (home_z // KV_HEADS == zi // KV_HEADS) & ((home_z != zi) | (j != y))
            nm_copies.append((leaves, copy))
            pl.when(leaves)(copy.start)

    @pl.when(is_home)
    def _():
        rows_in[head, span(home_piece * final, final), :] = grad_b[...]

    for e in range(2, z_count):
        spread_block(e)
    if both == 2:
        for e in range(1, z_count):
            with jax.named_scope(f'w_m2#{e}'):
                master_in(1, e).wait_recv()

        @pl.when(core == 1)
        def _():
            for e in range(1, min(z_count, 3)):
                second_block(e, beside)
    forward_block(1, both == 2)

    @pl.when(home_z != zi)
    def _():
        whole(base_in, BASE).wait_recv()

    with jax.named_scope('w_squares'):
        all_squares.wait_recv()
    square = own_square + jnp.sum(square_in[...], axis=0)
    rms = jnp.sqrt(square[:, 0:1] / (features * KV_HEADS * WIDE) + 1e-06)
    scale = 0.5 / rms
    row_me = row_of(y, x)

    @pl.loop(0, final // inner)
    def _(t):
        at = span(t * inner, inner)
        roll_ref[0, span(row_me + t * inner, inner), :] = (
            base_in[at, :].astype(jnp.float32) - scale * grad[at, :]).astype(jnp.bfloat16)

    parts = 2 if final // 2 % SUB == 0 else 1
    size = final // parts
    level_in = [[numbered() for _ in range(parts)] for _ in range(dims)]

    def layer0(yy, xx, u):
        return roll_ref.at[0, span(row_of(yy, xx) + u * size, size), :]

    def gather_in(i, u):
        return landing(roll_ref.at[0, pl.ds(0, size << (dims - 1 - i)), :], level_in[i][u])

    def gather_out(i, u):
        for at in have[:1 << (last - i)]:
            here = layer0(*at, u)
            put(here, here, partners[i], GATHER, level_in[i][u])

    def piece_out(at):
        for u in range(parts):
            here = layer0(*at, u)
            put(here, here, mate, PIECES, PIECES)

    have = [(y, x)]
    for i in reversed(range(dims)):
        have = have + [across(*at, i) for at in have]
    for u in range(parts):
        gather_out(last, u)
    piece_out(have[0])
    if relayed:
        for u in range(2):
            with jax.named_scope('w_relay'):
                landing(relay_in.at[pl.ds(u * (final // 2), final // 2)], relay_at[u]).wait_recv()
            pl.when(other_z != zi)(relay_out[u].start)

        @pl.when(other_z == zi)
        def _():
            rows_in[head] = relay_in[...]
    for e in range(2, z_count):
        forward_block(e, both == 2)
    if both == 2:
        @pl.when(core == 1)
        def _():
            for e in range(3, z_count):
                second_block(e, beside)
    for i in reversed(range(last)):
        for u in range(parts):
            with jax.named_scope(f'w_ag#{i + 1}#{u}'):
                gather_in(i + 1, u).wait_recv()
            gather_out(i, u)
        for at in have[1 << (last - 1 - i):1 << (last - i)]:
            piece_out(at)

    keeper = zi // half_z
    hand_in = [numbered() for _ in range(KV_HEADS)]
    hand_over = [copy_to(rows_in.at[h], rows_in.at[h], mate, HAND, hand_in[h]) for h in range(KV_HEADS)]

    def landed(h, p):
        return landing(rows_in.at[h, pl.ds(p * final, final)], nm_in + h * pieces + p)

    @pl.when(core == keeper)
    @jax.named_scope('w_rows')
    def _():
        low = zi + core * (z_count - 1 - 2 * zi)
        for h in range(KV_HEADS):
            for p in range(pieces):
                @pl.when((h != head) if relayed else (h != head) | (y != low * pieces + p))
                def _():
                    landed(h, p).wait_recv()
            hand_over[h].start()

    blocks = roll_ref.at[pl.ds(1, layer_count - 1), pl.ds(0, z_count * sub), :]
    if both == 2:
        with jax.named_scope('w_fwd'):
            whole(blocks, FORWARD).wait_recv()
        for z in near:
            for xx in (x, 1 - x):
                got = block(z, xx, 1 - yi)
                put(got, got, mate, TO_MATE, TO_MATE)
    with jax.named_scope('w_gathered'):
        for u in range(parts):
            gather_in(0, u).wait_recv()
            for at in have[n_rep // 2:]:
                here = layer0(*at, u)
                put(here, here, mate, PIECES, PIECES)

    @pl.when(core != keeper)
    @jax.named_scope('w_hand')
    def _():
        for copy in hand_over:
            copy.wait_recv()

    for h in range(KV_HEADS):
        for side in range(2):
            low = side * KV_HEADS * HEAD + h * HEAD
            nm_ref[:, low:low + HEAD] = (
                m0[:, low:low + HEAD] - scale * rows_in[h, :, side * HEAD:(side + 1) * HEAD].astype(jnp.float32))

    all_blocks = roll_ref.at[pl.ds(1, layer_count - 1), pl.ds(0, z_count * split * sub), :]
    all_pieces = roll_ref.at[0, pl.ds(0, n_rep * final), :]
    with jax.named_scope('w_mate'):
        whole(all_blocks, TO_MATE).wait_recv()
        whole(all_pieces, PIECES).wait_recv()

    @pl.when(core == keeper)
    def _():
        whole(rows_in, HAND).wait_send()

    @pl.when(is_home)
    def _():
        whole(zin.at[pl.ds(0, z_count - 1)], BASE).wait_send()

    for leaves, copy in nm_copies:
        pl.when(leaves)(copy.wait_send)
    for copy in mate_copies:
        copy.wait_send()
    whole(roll_ref.at[pl.ds(1, layer_count - 1), pl.ds(0, (z_count - 1) * both * sub), :], MASTERS).wait_send()
    whole(blocks, SPREAD).wait_send()
    if both == 2:
        whole(blocks, FORWARD).wait_send()
    if relayed:
        whole(relay_in, RELAY).wait_send()
    whole(all_blocks, TO_MATE).wait_send()
    whole(all_pieces, PIECES).wait_send()
    whole(roll_ref.at[0, pl.ds(0, (n_rep - 1) * final), :], GATHER).wait_send()
    whole(part.at[:, :, pl.ds(0, half - final), :], HALVES).wait_send()
    whole(zin.at[pl.ds(0, z_count - 1)], GRADS).wait_send()
    stats.wait_send()
    all_squares.wait_send()


def per_device(
    n_rep, n_shard, hidden, cotangent, seq_ids, response_mask, group_ids, rewards, new_logp, old_logp, ref_logp,
    master,
):
    everyone = n_rep * n_shard
    groups = everyone * SEQ_DEV // 8
    wide = -(-3 * groups // LANES) * LANES
    toks, features = hidden.shape
    layer_count, rows, cols = master.shape
    z_count = n_shard // 2
    split = 4 if n_rep % 4 == 0 and (rows // 4) % SUB == 0 else 2
    sub = rows // split
    half = features // 2
    final = half // n_rep
    pad = -(-toks // LANES) * LANES
    bf16, f32 = jnp.bfloat16, jnp.float32
    vmem, hbm = pl.BlockSpec(memory_space=pltpu.VMEM), pl.BlockSpec(memory_space=pltpu.HBM)
    dims = n_rep.bit_length() - 1
    both = 2 if split == 4 else 1
    landings = 7 + 4 + 2 + 4 + KV_HEADS + both * (z_count - 1) + z_count + 8 * dims + 2 * (z_count - 1) + KV_HEADS * (n_rep // z_count) + 2 * dims
    return pl.pallas_call(
        functools.partial(step_kernel, n_rep, n_shard, split, groups),
        out_shape=(pltpu.VMEM((rows, cols), f32), pltpu.VMEM((layer_count, features, WIDE), bf16)),
        in_specs=[hbm] * 10,
        out_specs=(vmem, vmem),
        scratch_shapes=[
            pltpu.SMEM((1, SEQ_DEV), jnp.int32),
            pltpu.SMEM((1, SEQ_DEV), f32),
            pltpu.VMEM((2, toks), jnp.int32),
            pltpu.VMEM((3, toks), f32),
            pltpu.VMEM((2, 1, wide), f32),
            pltpu.VMEM((everyone - 1, 1, wide), f32),
            pltpu.VMEM((everyone - 1, 1, LANES), f32),
            pltpu.VMEM((8, wide), f32),
            pltpu.VMEM((8, wide), f32),
            pltpu.VMEM((8, pad), f32),
            pltpu.VMEM((8, pad), f32),
            pltpu.VMEM((2 * toks, half), bf16),
            pltpu.VMEM((half, 2 * toks), bf16),
            pltpu.VMEM((2, toks, cols), bf16),
            pltpu.VMEM((2 * toks, WIDE), bf16),
            pltpu.VMEM((KV_HEADS, 2, half, HEAD), bf16),
            pltpu.VMEM((KV_HEADS, 2, half, HEAD), bf16),
            pltpu.VMEM((z_count + 1, 2, final, HEAD), bf16),
            pltpu.VMEM((final, WIDE), f32),
            pltpu.VMEM((final, WIDE), bf16),
            pltpu.VMEM((final, WIDE), bf16),
            pltpu.VMEM((KV_HEADS, final, WIDE), bf16),
            pltpu.VMEM((final, WIDE), bf16),
            pltpu.VMEM((rows, cols), f32),
            pltpu.VMEM((2, layer_count - 1, sub, cols), f32),
            pltpu.VMEM((2, KV_HEADS, layer_count - 1, sub, WIDE), bf16),
            pltpu.VMEM((KV_HEADS, rows, WIDE), bf16),
            pltpu.SemaphoreType.DMA((12,)),
            pltpu.SemaphoreType.DMA((4,)),
            pltpu.SemaphoreType.DMA((16 + n_rep // 2,)),
            pltpu.SemaphoreType.DMA((landings,)),
        ],
        compiler_params=pltpu.CompilerParams(
            collective_id=0, has_side_effects=True, vmem_limit_bytes=44 * 2**20
        ),
        name="step",
    )(*(pltpu.with_memory_space_constraint(value, pltpu.HBM) for value in (
        group_ids, rewards, seq_ids, response_mask, new_logp, old_logp, ref_logp, hidden, cotangent, master)))


def solution(mesh):
    tokens = P(("rep", "shard"), None)
    return jax.shard_map(
        functools.partial(per_device, mesh.shape["rep"], mesh.shape["shard"]),
        mesh=mesh,
        in_specs=(tokens,) * 9 + (P(None, "shard", None),),
        out_specs=(P("shard", None), P(None, None, "shard")),
        check_vma=False,
    )
```

```python
import functools

import jax
import jax.numpy as jnp
from jax import lax
from jax.experimental import pallas as pl
from jax.experimental.pallas import tpu as pltpu
from jax.sharding import PartitionSpec as P

HEAD = 128
KV_HEADS = 4
SEQ_DEV = 4
WIDE = 2 * HEAD
LANES = 128
SUB = 16
MESH = pl.DeviceIdType.MESH


def token_rows(seq_row, mask_row, new_row, old_row, ref_row):
    maskf = mask_row.astype(jnp.float32)
    onehot = [(seq_row == j).astype(jnp.float32) for j in range(SEQ_DEV)]
    tok_len = jnp.zeros_like(maskf)
    for hot in onehot:
        tok_len = tok_len + hot * jnp.maximum(jnp.sum(maskf * hot, axis=1, keepdims=True), 1.0)
    weight = maskf / tok_len
    ratio = -weight * jnp.exp(new_row - old_row)
    return [hot * ratio for hot in onehot] + [weight * (0.2 * (1.0 - jnp.exp(ref_row - new_row)))]


def flip(index, bit):
    step = 1 << bit
    here = (index // step) % 2
    return index + (1 - 2 * here) * step, here


def step_kernel(
    n_rep, n_shard, split, groups, group_hbm, reward_hbm, *args,
):
    token_hbm, args = args[:5], args[5:]
    step_body(n_rep, n_shard, split, groups, group_hbm, reward_hbm, token_hbm, *args)


def step_body(
    n_rep, n_shard, split, groups, group_hbm, reward_hbm, token_hbm,
    hidden_ref, cot_ref, master_ref,
    nm_ref, roll_ref,
    group_ref, reward_ref, ids_in, logp_in, small, stat_in, square_in, info_in, info_own, token_own, token_in, hid, hid_t, cot, delta, part, sums, zin,
    grad, grad_b, relay_in, base_out, base_in, m0, stage_in, stage_out, rows_in,
    local_sems, all_sems, set_send, set_recv,
):
    z_count = n_shard // 2
    dims = n_rep.bit_length() - 1
    everyone = n_rep * n_shard
    r, s = lax.axis_index("rep"), lax.axis_index("shard")
    me = r * n_shard + s
    core, y, x, zi = r % 2, r // 2, s % 2, s // 2
    head = zi % KV_HEADS
    toks, features = hidden_ref.shape
    half = features // 2
    layer_count, rows, cols = master_ref.shape
    sub = rows // split
    final = half // n_rep
    pieces = rows // final
    half_z = z_count // 2
    counter = [0]
    (SPREAD, FORWARD, TO_MATE, PIECES, BASE, RELAY, HAND,
     MASTERS, GATHER, HALVES, GRADS, RETURN) = range(12)
    given_in, given_out = 7, 12
    mate = (flip(r, 0)[0], s)

    def numbered():
        number = given_in + counter[0]
        counter[0] += 1
        return number

    def copy_to(src, dst, device, gone, landed):
        return pltpu.make_async_remote_copy(
            src_ref=src, dst_ref=dst, send_sem=set_send.at[gone], recv_sem=set_recv.at[landed],
            device_id=device, device_id_type=MESH)

    def put(src, dst, device, gone, landed):
        copy_to(src, dst, device, gone, landed).start()

    def whole(ref, number):
        return copy_to(ref, ref, mate, number, number)

    def landing(ref, number):
        return copy_to(ref, ref, mate, 0, number)

    def local(src, dst, number):
        copy = pltpu.make_async_copy(src, dst, local_sems.at[number])
        copy.start()
        return copy

    def span(at, size):
        return pl.ds(pl.multiple_of(at, SUB), size)

    def to_all(src, dst, sem):
        @pl.loop(1, everyone)
        def _(i):
            peer = (me + i) % everyone
            pltpu.make_async_remote_copy(
                src_ref=src, dst_ref=dst.at[i - 1], send_sem=all_sems.at[sem], recv_sem=all_sems.at[sem + 1],
                device_id=(peer // n_shard, peer % n_shard), device_id_type=MESH).start()

        return pltpu.make_async_remote_copy(
            src_ref=dst, dst_ref=dst, send_sem=all_sems.at[sem], recv_sem=all_sems.at[sem + 1],
            device_id=(flip(r, 0)[0], s), device_id_type=MESH)

    options = []
    for bit in range(1, dims):
        other, here = flip(r, bit)
        options.append((other, s, here))
    other, here = flip(s, 0)
    options.append((r, other, here))
    partners, bits = [], []
    for i in range(dims):
        a, b = options[i], options[(i + 1) % dims]
        partners.append(tuple(a[k] + core * (b[k] - a[k]) for k in range(2)))
        bits.append(a[2] + core * (b[2] - a[2]))
    z_peers = [None] + [(r, ((zi + d) % z_count) * 2 + x) for d in range(1, z_count)]

    def home(yy):
        low = yy // pieces
        return low + core * (z_count - 1 - 2 * low), yy % pieces

    def row_of(yy, xx):
        z, piece = home(yy)
        return (2 * z + xx) * rows + piece * final

    def across(yy, xx, i):
        moved = []
        for option in (i % dims, (i + 1) % dims):
            moved.append((flip(yy, option)[0], xx) if option < dims - 1 else (yy, 1 - xx))
        (ya, xa), (yb, xb) = moved
        return ya + core * (yb - ya), xa + core * (xb - xa)

    def spot(j, c):
        low, xx, piece = j // pieces // 2, j // pieces % 2, j % pieces
        yy = (low if c == 0 else half_z - 1 - low) * pieces + piece
        chosen = [(yy >> o) & 1 for o in range(dims - 1)] + [xx]
        return sum(chosen[(i + c) % dims] << (dims - 1 - i) for i in range(dims))

    home_z, home_piece = home(y)
    quarter = r % split
    own_half = pl.ds(pl.multiple_of(core * half, LANES), half)
    other_half = pl.ds(pl.multiple_of((1 - core) * half, LANES), half)
    yi = quarter // 2
    both = 2 if split == 4 else 1
    quarters = [quarter, quarter + (1 - 2 * yi) * 2][:both]
    fetch_stage = [
        local(master_ref.at[pl.ds(1, layer_count - 1), span(q * sub, sub), :], stage_in.at[n], (0, 11)[n])
        for n, q in enumerate(quarters)]
    fetch_hid = local(hidden_ref.at[:, own_half], hid.at[pl.ds(0, toks)], 1)
    fetch_cot = local(cot_ref, cot.at[0], 2)
    fetch_m0 = local(master_ref.at[0], m0, 3)
    fetch_small = [local(group_hbm, group_ref, 4), local(reward_hbm, reward_ref, 5)]
    fetch_tokens = [local(ref, ids_in.at[pl.ds(n, 1)], 6 + n) for n, ref in enumerate(token_hbm[:2])]
    fetch_tokens += [local(ref, logp_in.at[pl.ds(n, 1)], 8 + n) for n, ref in enumerate(token_hbm[2:])]

    barrier = pltpu.get_barrier_semaphore()

    @pl.loop(1, everyone)
    def _(i):
        peer = (me + i) % everyone
        pl.semaphore_signal(
            barrier, inc=1, device_id=(peer // n_shard, peer % n_shard), device_id_type=MESH)

    shape = info_in.shape
    line = lax.broadcasted_iota(jnp.int32, shape, 0)
    lane = lax.broadcasted_iota(jnp.int32, shape, 1)
    row_lane = lax.broadcasted_iota(jnp.int32, (1, shape[1]), 1)
    info = jnp.zeros(shape, jnp.float32)
    own_sums = jnp.zeros((1, shape[1]), jnp.float32)
    for copy in fetch_small:
        copy.wait()
    for j in range(SEQ_DEV):
        group, given = group_ref[0, j], reward_ref[0, j]
        info = jnp.where((line == j) & (lane == group), 1.0, info)
        info = jnp.where(line == SEQ_DEV + j, given, info)
        for n, value in enumerate((1.0, given, given * given)):
            own_sums = own_sums + jnp.where(row_lane == n * groups + group, value, 0.0)
    info_own[...] = info
    small[0] = own_sums
    token_own[...] = jnp.zeros_like(token_own)
    with jax.named_scope('w_barrier'):
        pl.semaphore_wait(barrier, everyone - 1)

    stats = to_all(small.at[0], stat_in, 0)
    sent_out = n_rep // 2 + given_out
    mate_copies = [
        copy_to(src, dst, mate, sent_out + n, numbered()) for n, (src, dst) in enumerate((
            (info_own, info_in), (hidden_ref.at[:, other_half], hid.at[pl.ds(toks, toks)]), (cot_ref, cot.at[1]),
            (token_own, token_in)))]
    mate_info, mate_hid, mate_cot, mate_tok = mate_copies
    for copy in mate_copies[:3]:
        copy.start()

    def block(z, xx, yy):
        return roll_ref.at[pl.ds(1, layer_count - 1), span((2 * z + xx) * rows + (2 * yy + core) * sub, sub), :]

    near = [zi]
    for e in range(1, z_count):
        z = zi
        for bit in range(z_count.bit_length() - 1):
            if e >> bit & 1:
                z = flip(z, bit)[0]
        near.append(z)
    beside = (r, flip(s, 0)[0])
    above = (flip(r, 1)[0], s)
    halves_at = [yi, 1 - yi]
    m1 = [[numbered() for _ in range(1, z_count)] for _ in range(both)]

    def master_in(n, e):
        return landing(block(zi, x, halves_at[n]), m1[n][e - 1])

    def stage_masters(n):
        with jax.named_scope('w_stage'):
            fetch_stage[n].wait()
        for h in range(KV_HEADS):
            low = KV_HEADS * HEAD + h * HEAD
            for l in range(layer_count - 1):
                stage_out[n, h, l, :, :HEAD] = stage_in[n, l, :, h * HEAD:(h + 1) * HEAD].astype(jnp.bfloat16)
                stage_out[n, h, l, :, HEAD:] = stage_in[n, l, :, low:low + HEAD].astype(jnp.bfloat16)
        roll_ref[1:, span((2 * zi + x) * rows + quarters[n] * sub, sub), :] = stage_out[n, head]

    def send_masters(n, which):
        for e in which:
            put(stage_out.at[n, near[e] % KV_HEADS], block(zi, x, halves_at[n]), (r, near[e] * 2 + x),
                MASTERS, m1[n][e - 1])

    stage_masters(0)
    send_masters(0, range(1, z_count))
    spread_in = [numbered() for _ in range(z_count)]

    def second_block(e, device):
        here = block(near[e], x, 1 - yi)
        put(here, here, device, FORWARD, FORWARD)

    def spread_block(e):
        if e:
            with jax.named_scope(f'w_m1#{e}'):
                master_in(0, e).wait_recv()
        here = block(near[e], x, yi)
        put(here, here, beside, SPREAD, spread_in[e])
        put(here, here, mate, TO_MATE, TO_MATE)

    def forward_block(e, up):
        got = block(near[e], 1 - x, yi)
        with jax.named_scope(f'w_sp#{e}'):
            landing(got, spread_in[e]).wait_recv()
        if up:
            @pl.when(core == 0)
            def _():
                put(got, got, above, FORWARD, FORWARD)
        put(got, got, mate, TO_MATE, TO_MATE)

    spread_block(0)

    for copy in fetch_tokens:
        copy.wait()
    terms = token_rows(ids_in[0:1], ids_in[1:2], logp_in[0:1], logp_in[1:2], logp_in[2:3])
    for j, row in enumerate(terms):
        token_own[j:j + 1, :toks] = row
    mate_tok.start()
    if both == 2:
        stage_masters(1)
        second_block(0, beside)

    is_home = home_z == zi
    fetch_m0.wait()

    @pl.when(is_home)
    def _():
        at = span(home_piece * final, final)
        for h in range(KV_HEADS):
            low = KV_HEADS * HEAD + h * HEAD
            base_out[h, :, :HEAD] = m0[at, h * HEAD:(h + 1) * HEAD].astype(jnp.bfloat16)
            base_out[h, :, HEAD:] = m0[at, low:low + HEAD].astype(jnp.bfloat16)
        for d in range(1, z_count):
            put(base_out.at[(head + d) % KV_HEADS], base_in, z_peers[d], BASE, BASE)
        base_in[...] = base_out[head]

    with jax.named_scope('w_hid'):
        fetch_hid.wait()
        mate_hid.wait_recv()

    @pl.loop(0, half // WIDE)
    def _(t):
        at = pl.multiple_of(t * WIDE, WIDE)
        hid_t[pl.ds(at, WIDE), :] = jnp.transpose(hid[:, pl.ds(at, WIDE)])

    with jax.named_scope('w_cot'):
     fetch_cot.wait()
    mate_cot.wait_recv()
    mate_info.wait_recv()
    mate_tok.wait_recv()
    with jax.named_scope('w_stats'):
        stats.wait_recv()
    total = own_sums + jnp.sum(stat_in[...], axis=0)
    wide = shape[1]
    count = jnp.maximum(total, 1.0)
    mean = pltpu.roll(total, wide - groups, 1) / count
    spread_of = jnp.maximum(
        jnp.sqrt(jnp.maximum(pltpu.roll(total, wide - 2 * groups, 1) / count - mean * mean, 0.0)), 0.5)

    def coef_of(told, token):
        hots, given = told[:SEQ_DEV], told[SEQ_DEV:, 0:1]
        advantage = (given - jnp.sum(hots * mean, axis=1, keepdims=True)) / jnp.sum(
            hots * spread_of, axis=1, keepdims=True)
        out = token[SEQ_DEV:SEQ_DEV + 1]
        for j in range(SEQ_DEV):
            out = out + token[j:j + 1] * advantage[j:j + 1]
        return jnp.transpose(jnp.broadcast_to(out, (LANES, out.shape[1])))[:toks]

    coefs = [coef_of(info, token_own[...]), coef_of(info_in[...], token_in[...])]

    lens, offsets = [half], [0]
    for i in range(dims):
        lens.append(lens[-1] // 2)
        offsets.append(offsets[-1] + bits[i] * lens[-1])
    starts, at = [], 0
    for length in lens[1:]:
        starts.append(at)
        at += length
    turns = [2, 1, 3, 0]
    order = [(head + d) % KV_HEADS for d in turns]
    paired = z_count == KV_HEADS
    pair_z = flip(zi, 0)[0]
    inner_plane = (zi + 1) // 2 % 2 == 1
    if paired:
        outer_z = (1 - zi // 2) * 3
        order = [outer_z, flip(outer_z, 0)[0], pair_z, zi]
    tile = half // 2
    chunks = 2 * KV_HEADS
    inbound = {(i, k): numbered() for i in range(dims) for k in range(chunks)}

    def halves(i, k):
        gone = offsets[i] + (1 - bits[i]) * lens[i + 1]
        return pltpu.make_async_remote_copy(
            src_ref=part.at[order[k // 2], k % 2, span(gone, lens[i + 1])],
            dst_ref=sums.at[order[k // 2], k % 2, pl.ds(starts[i], lens[i + 1])],
            send_sem=set_send.at[HALVES], recv_sem=set_recv.at[inbound[i, k]],
            device_id=partners[i], device_id_type=MESH)

    def pass_on(i, k):
        halves(i, k).start()

    def multiply_at(h, top, n):
        where = [[[spot(j, c) for j in range(n_rep)].index(b * (n_rep // 2) + n) for b in range(2)] for c in range(2)]
        (a, b), (a1, b1) = where
        low, high = a + core * (a1 - a), b + core * (b1 - b)
        out = jnp.dot(
            hid_t[span((low + top * (high - low)) * final, final), :], delta[...], preferred_element_type=jnp.float32
        ).astype(jnp.bfloat16)
        at = span((top * (n_rep // 2) + n) * final, final)
        for side in range(2):
            part[h, side, at, :] = out[:, side * HEAD:(side + 1) * HEAD]

    for k in range(KV_HEADS):
        h = order[k]
        for side in range(2):
            low = pl.ds(pl.multiple_of(side * KV_HEADS * HEAD + h * HEAD, HEAD), HEAD)
            for src in range(2):
                delta[src * toks:(src + 1) * toks, side * HEAD:(side + 1) * HEAD] = (
                    coefs[src] * cot[src, :, low].astype(jnp.float32)).astype(jnp.bfloat16)
        if k == 0:
            for stays in (0, 1):
                for n in range(n_rep // 2):
                    multiply_at(h, bits[0] if stays else 1 - bits[0], n)
                if not stays:
                    pass_on(0, 0)
                    pass_on(0, 1)
            continue
        for t in range(2):
          with jax.named_scope(f'mul#k={k}'):
            out = jnp.dot(
                hid_t[t * tile:(t + 1) * tile, :], delta[...], preferred_element_type=jnp.float32
            ).astype(jnp.bfloat16)
            for q in range(tile // final):
                j = t * (tile // final) + q
                place = spot(j, 0) + core * (spot(j, 1) - spot(j, 0))
                for side in range(2):
                    part[h, side, span(place * final, final), :] = (
                        out[q * final:(q + 1) * final, side * HEAD:(side + 1) * HEAD])
        pass_on(0, 2 * k)
        pass_on(0, 2 * k + 1)
    spread_block(1)
    if both == 2:
        send_masters(1, [e for e in range(1, z_count) if e != 2])

    inner = min(final, 112)

    def add_in(i, k):
        h, side = order[k // 2], k % 2

        @pl.loop(0, lens[i + 1] // inner)
        def _(t):
            at = span(offsets[i + 1] + t * inner, inner)
            part[h, side, at, :] = (
                part[h, side, at, :].astype(jnp.float32)
                + sums[h, side, span(starts[i] + t * inner, inner), :].astype(jnp.float32)
            ).astype(jnp.bfloat16)

    last = dims - 1
    mine = span(offsets[dims], final)
    sources = range(2) if paired else range(z_count - 1)
    z_in = {(n, side): numbered() for side in range(2) for n in sources}
    z_mid = [numbered() for _ in range(4)] if paired else []

    def z_put(k, landing_ref, number, z):
        put(part.at[order[k // 2], k % 2, mine], landing_ref, (r, 2 * z + x), GRADS, number)

    def z_send(k):
        if not paired:
            for d in range(1, z_count):
                if d % KV_HEADS == turns[k // 2]:
                    z_put(k, zin.at[d - 1, k % 2], z_in[d - 1, k % 2], (zi + d) % z_count)
        elif k < 4:
            @pl.when(jnp.logical_not(inner_plane))
            def _():
                z_put(k, zin.at[3 + k // 2, k % 2], z_mid[k], pair_z)
        elif k < 6:
            z_put(k, zin.at[1, k % 2], z_in[1, k % 2], pair_z)

    def z_combine(k):
        held = zin.at[3 + k // 2, k % 2]

        @pl.when(inner_plane)
        def _():
            with jax.named_scope(f'w_mid#{k}'):
                landing(held, z_mid[k]).wait_recv()
            h, side = order[k // 2], k % 2
            part[h, side, mine, :] = (
                part[h, side, mine, :].astype(jnp.float32) + held[...].astype(jnp.float32)).astype(jnp.bfloat16)
            z_put(k, zin.at[0, k % 2], z_in[0, k % 2], order[k // 2])

    far = z_count > KV_HEADS
    squares = {}

    def own_sum(side):
        for n in sources:
            with jax.named_scope(f'w_z#{n}'):
                landing(zin.at[n, side], z_in[n, side]).wait_recv()
        g = part[head, side, mine, :].astype(jnp.float32)
        if not far:
            g = g + sums[head, side, pl.ds(starts[last], final), :].astype(jnp.float32)
        for n in sources:
            g = g + zin[n, side].astype(jnp.float32)
        cut = slice(side * HEAD, (side + 1) * HEAD)
        grad[:, cut] = g
        grad_b[:, cut] = g.astype(jnp.bfloat16)
        squares[side] = jnp.sum(g * g, axis=0, keepdims=True)

    for t in range(chunks + last):
        for k in range(4 if paired else 0):
            if t == last + (3, 4, 5, 5)[k]:
                z_combine(k)
        for i in range(dims):
            k = t - i
            if k < 0 or k >= chunks:
                continue
            with jax.named_scope(f'w_in#i={i}#k={k}'):
                halves(i, k).wait_recv()
            if i == last and k // 2 == KV_HEADS - 1 and not far:
                own_sum(k % 2)
                continue
            add_in(i, k)
            if i < last:
                pass_on(i + 1, k)
            else:
                z_send(k)
        if both == 2 and t == 6 and z_count > 2:
            send_masters(1, [2])
        if t == 5:
            forward_block(0, False)
    if far:
        for side in range(2):
            own_sum(side)
    own_square = squares[0] + squares[1]
    own_square = jnp.broadcast_to(jnp.sum(own_square, axis=1, keepdims=True), (1, LANES))
    small[1, :, :LANES] = own_square
    all_squares = to_all(small.at[1, :, pl.ds(0, LANES)], square_in, 2)

    relayed = n_rep == 4 and pieces == 1
    relay_at = [numbered(), numbered()]
    y_other = flip(y, 0)[0] if relayed else y
    other_z = home(y_other)[0]
    nm_in = [numbered() for _ in range(KV_HEADS * pieces)][0]
    here_rows = rows_in.at[head, span(home_piece * final, final)]
    if relayed:
        for u in range(2):
            cut = pl.ds(u * (final // 2), final // 2)
            put(grad_b.at[cut], relay_in.at[cut], above, RELAY, relay_at[u])
        nm_copies = [
            (home_z != zi, copy_to(grad_b, here_rows, (r, 2 * home_z + x), RETURN, nm_in + head)),
            (other_z != zi, copy_to(relay_in, here_rows, (r, 2 * other_z + x), RETURN + 1, nm_in + head))]
        relay_out = [
            copy_to(relay_in.at[pl.ds(u * (final // 2), final // 2)],
                    rows_in.at[head, pl.ds(u * (final // 2), final // 2)],
                    (r, 2 * other_z + x), RETURN + 1, nm_in + head)
            for u in range(2)]
        pl.when(home_z != zi)(nm_copies[0][1].start)
    else:
        nm_copies = []
        for j in range(n_rep // 2):
            copy = copy_to(
                grad_b, here_rows, (2 * j + core, 2 * home_z + x),
                RETURN + j, nm_in + head * pieces + home_piece)
            leaves = (home_z // KV_HEADS == zi // KV_HEADS) & ((home_z != zi) | (j != y))
            nm_copies.append((leaves, copy))
            pl.when(leaves)(copy.start)

    @pl.when(is_home)
    def _():
        rows_in[head, span(home_piece * final, final), :] = grad_b[...]

    for e in range(2, z_count):
        spread_block(e)
    if both == 2:
        for e in range(1, z_count):
            with jax.named_scope(f'w_m2#{e}'):
                master_in(1, e).wait_recv()

        @pl.when(core == 1)
        def _():
            for e in range(1, min(z_count, 3)):
                second_block(e, beside)
    forward_block(1, both == 2)

    @pl.when(home_z != zi)
    def _():
        whole(base_in, BASE).wait_recv()

    with jax.named_scope('w_squares'):
        all_squares.wait_recv()
    square = own_square + jnp.sum(square_in[...], axis=0)
    rms = jnp.sqrt(square[:, 0:1] / (features * KV_HEADS * WIDE) + 1e-06)
    scale = 0.5 / rms
    row_me = row_of(y, x)

    @pl.loop(0, final // inner)
    def _(t):
        at = span(t * inner, inner)
        roll_ref[0, span(row_me + t * inner, inner), :] = (
            base_in[at, :].astype(jnp.float32) - scale * grad[at, :]).astype(jnp.bfloat16)

    parts = 4 if final // 4 % SUB == 0 else 1
    size = final // parts
    level_in = [[numbered() for _ in range(parts)] for _ in range(dims)]

    def layer0(yy, xx, u):
        return roll_ref.at[0, span(row_of(yy, xx) + u * size, size), :]

    def gather_in(i, u):
        return landing(roll_ref.at[0, pl.ds(0, size << (dims - 1 - i)), :], level_in[i][u])

    def gather_out(i, u):
        for at in have[:1 << (last - i)]:
            here = layer0(*at, u)
            put(here, here, partners[i], GATHER, level_in[i][u])

    def piece_out(at):
        for u in range(parts):
            here = layer0(*at, u)
            put(here, here, mate, PIECES, PIECES)

    have = [(y, x)]
    for i in reversed(range(dims)):
        have = have + [across(*at, i) for at in have]
    for u in range(parts):
        gather_out(last, u)
    piece_out(have[0])
    if relayed:
        for u in range(2):
            with jax.named_scope('w_relay'):
                landing(relay_in.at[pl.ds(u * (final // 2), final // 2)], relay_at[u]).wait_recv()
            pl.when(other_z != zi)(relay_out[u].start)

        @pl.when(other_z == zi)
        def _():
            rows_in[head] = relay_in[...]
    for e in range(2, z_count):
        forward_block(e, both == 2)
    if both == 2:
        @pl.when(core == 1)
        def _():
            for e in range(3, z_count):
                second_block(e, beside)
    for i in reversed(range(last)):
        for u in range(parts):
            with jax.named_scope(f'w_ag#{i + 1}#{u}'):
                gather_in(i + 1, u).wait_recv()
            gather_out(i, u)
        for at in have[1 << (last - 1 - i):1 << (last - i)]:
            piece_out(at)

    keeper = zi // half_z
    hand_in = [numbered() for _ in range(KV_HEADS)]
    hand_over = [copy_to(rows_in.at[h], rows_in.at[h], mate, HAND, hand_in[h]) for h in range(KV_HEADS)]

    def landed(h, p):
        return landing(rows_in.at[h, pl.ds(p * final, final)], nm_in + h * pieces + p)

    @pl.when(core == keeper)
    @jax.named_scope('w_rows')
    def _():
        low = zi + core * (z_count - 1 - 2 * zi)
        for h in range(KV_HEADS):
            for p in range(pieces):
                @pl.when((h != head) if relayed else (h != head) | (y != low * pieces + p))
                def _():
                    landed(h, p).wait_recv()
            hand_over[h].start()

    blocks = roll_ref.at[pl.ds(1, layer_count - 1), pl.ds(0, z_count * sub), :]
    if both == 2:
        with jax.named_scope('w_fwd'):
            whole(blocks, FORWARD).wait_recv()
        for z in near:
            for xx in (x, 1 - x):
                got = block(z, xx, 1 - yi)
                put(got, got, mate, TO_MATE, TO_MATE)
    with jax.named_scope('w_gathered'):
        for u in range(parts):
            gather_in(0, u).wait_recv()
            for at in have[n_rep // 2:]:
                here = layer0(*at, u)
                put(here, here, mate, PIECES, PIECES)

    @pl.when(core != keeper)
    @jax.named_scope('w_hand')
    def _():
        for copy in hand_over:
            copy.wait_recv()

    for h in range(KV_HEADS):
        for side in range(2):
            low = side * KV_HEADS * HEAD + h * HEAD
            nm_ref[:, low:low + HEAD] = (
                m0[:, low:low + HEAD] - scale * rows_in[h, :, side * HEAD:(side + 1) * HEAD].astype(jnp.float32))

    all_blocks = roll_ref.at[pl.ds(1, layer_count - 1), pl.ds(0, z_count * split * sub), :]
    all_pieces = roll_ref.at[0, pl.ds(0, n_rep * final), :]
    with jax.named_scope('w_mate'):
        whole(all_blocks, TO_MATE).wait_recv()
        whole(all_pieces, PIECES).wait_recv()

    @pl.when(core == keeper)
    def _():
        whole(rows_in, HAND).wait_send()

    @pl.when(is_home)
    def _():
        whole(zin.at[pl.ds(0, z_count - 1)], BASE).wait_send()

    for leaves, copy in nm_copies:
        pl.when(leaves)(copy.wait_send)
    for copy in mate_copies:
        copy.wait_send()
    whole(roll_ref.at[pl.ds(1, layer_count - 1), pl.ds(0, (z_count - 1) * both * sub), :], MASTERS).wait_send()
    whole(blocks, SPREAD).wait_send()
    if both == 2:
        whole(blocks, FORWARD).wait_send()
    if relayed:
        whole(relay_in, RELAY).wait_send()
    whole(all_blocks, TO_MATE).wait_send()
    whole(all_pieces, PIECES).wait_send()
    whole(roll_ref.at[0, pl.ds(0, (n_rep - 1) * final), :], GATHER).wait_send()
    whole(part.at[:, :, pl.ds(0, half - final), :], HALVES).wait_send()
    whole(zin.at[pl.ds(0, z_count - 1)], GRADS).wait_send()
    stats.wait_send()
    all_squares.wait_send()


def copy_kernel(nm_ref, roll_ref, nm_out, roll_out, sems):
    layer_count, features, _ = roll_ref.shape
    copies = [pltpu.make_async_copy(nm_ref, nm_out, sems.at[0])]
    for l in range(layer_count):
        for n in range(2):
            cut = pl.ds(n * (features // 2), features // 2)
            copies.append(pltpu.make_async_copy(
                roll_ref.at[l, cut], roll_out.at[l, cut], sems.at[1 + 2 * l + n]))
    for copy in copies:
        copy.start()
    for copy in copies:
        copy.wait()


def per_device(
    n_rep, n_shard, hidden, cotangent, seq_ids, response_mask, group_ids, rewards, new_logp, old_logp, ref_logp,
    master,
):
    everyone = n_rep * n_shard
    groups = everyone * SEQ_DEV // 8
    wide = -(-3 * groups // LANES) * LANES
    toks, features = hidden.shape
    layer_count, rows, cols = master.shape
    z_count = n_shard // 2
    split = 4 if n_rep % 4 == 0 and (rows // 4) % SUB == 0 else 2
    sub = rows // split
    half = features // 2
    final = half // n_rep
    pad = -(-toks // LANES) * LANES
    bf16, f32 = jnp.bfloat16, jnp.float32
    vmem, hbm = pl.BlockSpec(memory_space=pltpu.VMEM), pl.BlockSpec(memory_space=pltpu.HBM)
    dims = n_rep.bit_length() - 1
    both = 2 if split == 4 else 1
    landings = 7 + 4 + 2 + 4 + KV_HEADS + both * (z_count - 1) + z_count + 8 * dims + 2 * (z_count - 1) + KV_HEADS * (n_rep // z_count) + 4 * dims
    results = pl.pallas_call(
        functools.partial(step_kernel, n_rep, n_shard, split, groups),
        out_shape=(pltpu.VMEM((rows, cols), f32), pltpu.VMEM((layer_count, features, WIDE), bf16)),
        in_specs=[hbm] * 10,
        out_specs=(vmem, vmem),
        scratch_shapes=[
            pltpu.SMEM((1, SEQ_DEV), jnp.int32),
            pltpu.SMEM((1, SEQ_DEV), f32),
            pltpu.VMEM((2, toks), jnp.int32),
            pltpu.VMEM((3, toks), f32),
            pltpu.VMEM((2, 1, wide), f32),
            pltpu.VMEM((everyone - 1, 1, wide), f32),
            pltpu.VMEM((everyone - 1, 1, LANES), f32),
            pltpu.VMEM((8, wide), f32),
            pltpu.VMEM((8, wide), f32),
            pltpu.VMEM((8, pad), f32),
            pltpu.VMEM((8, pad), f32),
            pltpu.VMEM((2 * toks, half), bf16),
            pltpu.VMEM((half, 2 * toks), bf16),
            pltpu.VMEM((2, toks, cols), bf16),
            pltpu.VMEM((2 * toks, WIDE), bf16),
            pltpu.VMEM((KV_HEADS, 2, half, HEAD), bf16),
            pltpu.VMEM((KV_HEADS, 2, half, HEAD), bf16),
            pltpu.VMEM((z_count + 1, 2, final, HEAD), bf16),
            pltpu.VMEM((final, WIDE), f32),
            pltpu.VMEM((final, WIDE), bf16),
            pltpu.VMEM((final, WIDE), bf16),
            pltpu.VMEM((KV_HEADS, final, WIDE), bf16),
            pltpu.VMEM((final, WIDE), bf16),
            pltpu.VMEM((rows, cols), f32),
            pltpu.VMEM((2, layer_count - 1, sub, cols), f32),
            pltpu.VMEM((2, KV_HEADS, layer_count - 1, sub, WIDE), bf16),
            pltpu.VMEM((KV_HEADS, rows, WIDE), bf16),
            pltpu.SemaphoreType.DMA((12,)),
            pltpu.SemaphoreType.DMA((4,)),
            pltpu.SemaphoreType.DMA((16 + n_rep // 2,)),
            pltpu.SemaphoreType.DMA((landings,)),
        ],
        compiler_params=pltpu.CompilerParams(
            collective_id=0, has_side_effects=True, vmem_limit_bytes=44 * 2**20
        ),
        name="step",
    )(*(pltpu.with_memory_space_constraint(value, pltpu.HBM) for value in (
        group_ids, rewards, seq_ids, response_mask, new_logp, old_logp, ref_logp, hidden, cotangent, master)))
    return pl.pallas_call(
        copy_kernel,
        out_shape=tuple(jax.ShapeDtypeStruct(value.shape, value.dtype) for value in results),
        in_specs=[vmem] * 2,
        out_specs=(hbm, hbm),
        scratch_shapes=[pltpu.SemaphoreType.DMA((8,))],
        compiler_params=pltpu.CompilerParams(vmem_limit_bytes=2**20),
        name="copy",
    )(*(pltpu.with_memory_space_constraint(value, pltpu.VMEM) for value in results))


def solution(mesh):
    tokens = P(("rep", "shard"), None)
    return jax.shard_map(
        functools.partial(per_device, mesh.shape["rep"], mesh.shape["shard"]),
        mesh=mesh,
        in_specs=(tokens,) * 9 + (P(None, "shard", None),),
        out_specs=(P("shard", None), P(None, None, "shard")),
        check_vma=False,
    )
```

```python
import functools

import jax
import jax.numpy as jnp
from jax import lax
from jax.experimental import pallas as pl
from jax.experimental.pallas import tpu as pltpu
from jax.sharding import PartitionSpec as P

HEAD = 128
KV_HEADS = 4
SEQ_DEV = 4
WIDE = 2 * HEAD
LANES = 128
SUB = 16
MESH = pl.DeviceIdType.MESH


def token_rows(seq_row, mask_row, new_row, old_row, ref_row):
    maskf = mask_row.astype(jnp.float32)
    onehot = [(seq_row == j).astype(jnp.float32) for j in range(SEQ_DEV)]
    tok_len = jnp.zeros_like(maskf)
    for hot in onehot:
        tok_len = tok_len + hot * jnp.maximum(jnp.sum(maskf * hot, axis=1, keepdims=True), 1.0)
    weight = maskf / tok_len
    ratio = -weight * jnp.exp(new_row - old_row)
    return [hot * ratio for hot in onehot] + [weight * (0.2 * (1.0 - jnp.exp(ref_row - new_row)))]


def flip(index, bit):
    step = 1 << bit
    here = (index // step) % 2
    return index + (1 - 2 * here) * step, here


def step_kernel(
    n_rep, n_shard, split, groups, group_hbm, reward_hbm, *args,
):
    token_hbm, args = args[:5], args[5:]
    step_body(n_rep, n_shard, split, groups, group_hbm, reward_hbm, token_hbm, *args)


def step_body(
    n_rep, n_shard, split, groups, group_hbm, reward_hbm, token_hbm,
    hidden_ref, cot_ref, master_ref,
    nm_ref, roll_ref,
    group_ref, reward_ref, ids_in, logp_in, small, stat_in, square_in, info_in, info_own, token_own, token_in, hid, hid_t, cot, delta, part, sums, zin,
    grad, grad_b, relay_in, base_out, base_in, m0, stage_in, stage_out, rows_in,
    local_sems, all_sems, set_send, set_recv,
):
    z_count = n_shard // 2
    dims = n_rep.bit_length() - 1
    everyone = n_rep * n_shard
    r, s = lax.axis_index("rep"), lax.axis_index("shard")
    me = r * n_shard + s
    core, y, x, zi = r % 2, r // 2, s % 2, s // 2
    head = zi % KV_HEADS
    toks, features = hidden_ref.shape
    half = features // 2
    layer_count, rows, cols = master_ref.shape
    sub = rows // split
    final = half // n_rep
    pieces = rows // final
    half_z = z_count // 2
    counter = [0]
    (SPREAD, FORWARD, TO_MATE, PIECES, BASE, RELAY, HAND,
     MASTERS, GATHER, HALVES, GRADS, RETURN) = range(12)
    given_in, given_out = 7, 12
    mate = (flip(r, 0)[0], s)

    def numbered():
        number = given_in + counter[0]
        counter[0] += 1
        return number

    def copy_to(src, dst, device, gone, landed):
        return pltpu.make_async_remote_copy(
            src_ref=src, dst_ref=dst, send_sem=set_send.at[gone], recv_sem=set_recv.at[landed],
            device_id=device, device_id_type=MESH)

    def put(src, dst, device, gone, landed):
        copy_to(src, dst, device, gone, landed).start()

    def whole(ref, number):
        return copy_to(ref, ref, mate, number, number)

    def landing(ref, number):
        return copy_to(ref, ref, mate, 0, number)

    def local(src, dst, number):
        copy = pltpu.make_async_copy(src, dst, local_sems.at[number])
        copy.start()
        return copy

    def span(at, size):
        return pl.ds(pl.multiple_of(at, SUB), size)

    def to_all(src, dst, sem):
        @pl.loop(1, everyone)
        def _(i):
            peer = (me + i) % everyone
            pltpu.make_async_remote_copy(
                src_ref=src, dst_ref=dst.at[i - 1], send_sem=all_sems.at[sem], recv_sem=all_sems.at[sem + 1],
                device_id=(peer // n_shard, peer % n_shard), device_id_type=MESH).start()

        return pltpu.make_async_remote_copy(
            src_ref=dst, dst_ref=dst, send_sem=all_sems.at[sem], recv_sem=all_sems.at[sem + 1],
            device_id=(flip(r, 0)[0], s), device_id_type=MESH)

    options = []
    for bit in range(1, dims):
        other, here = flip(r, bit)
        options.append((other, s, here))
    other, here = flip(s, 0)
    options.append((r, other, here))
    partners, bits = [], []
    for i in range(dims):
        a, b = options[i], options[(i + 1) % dims]
        partners.append(tuple(a[k] + core * (b[k] - a[k]) for k in range(2)))
        bits.append(a[2] + core * (b[2] - a[2]))
    z_peers = [None] + [(r, ((zi + d) % z_count) * 2 + x) for d in range(1, z_count)]

    def home(yy):
        low = yy // pieces
        return low + core * (z_count - 1 - 2 * low), yy % pieces

    def row_of(yy, xx):
        z, piece = home(yy)
        return (2 * z + xx) * rows + piece * final

    def across(yy, xx, i):
        moved = []
        for option in (i % dims, (i + 1) % dims):
            moved.append((flip(yy, option)[0], xx) if option < dims - 1 else (yy, 1 - xx))
        (ya, xa), (yb, xb) = moved
        return ya + core * (yb - ya), xa + core * (xb - xa)

    def spot(j, c):
        low, xx, piece = j // pieces // 2, j // pieces % 2, j % pieces
        yy = (low if c == 0 else half_z - 1 - low) * pieces + piece
        chosen = [(yy >> o) & 1 for o in range(dims - 1)] + [xx]
        return sum(chosen[(i + c) % dims] << (dims - 1 - i) for i in range(dims))

    home_z, home_piece = home(y)
    quarter = r % split
    own_half = pl.ds(pl.multiple_of(core * half, LANES), half)
    other_half = pl.ds(pl.multiple_of((1 - core) * half, LANES), half)
    yi = quarter // 2
    both = 2 if split == 4 else 1
    quarters = [quarter, quarter + (1 - 2 * yi) * 2][:both]
    fetch_stage = [
        local(master_ref.at[pl.ds(1, layer_count - 1), span(q * sub, sub), :], stage_in.at[n], (0, 11)[n])
        for n, q in enumerate(quarters)]
    fetch_hid = local(hidden_ref.at[:, own_half], hid.at[pl.ds(0, toks)], 1)
    fetch_cot = local(cot_ref, cot.at[0], 2)
    fetch_m0 = local(master_ref.at[0], m0, 3)
    fetch_small = [local(group_hbm, group_ref, 4), local(reward_hbm, reward_ref, 5)]
    fetch_tokens = [local(ref, ids_in.at[pl.ds(n, 1)], 6 + n) for n, ref in enumerate(token_hbm[:2])]
    fetch_tokens += [local(ref, logp_in.at[pl.ds(n, 1)], 8 + n) for n, ref in enumerate(token_hbm[2:])]

    barrier = pltpu.get_barrier_semaphore()

    @pl.loop(1, everyone)
    def _(i):
        peer = (me + i) % everyone
        pl.semaphore_signal(
            barrier, inc=1, device_id=(peer // n_shard, peer % n_shard), device_id_type=MESH)

    shape = info_in.shape
    line = lax.broadcasted_iota(jnp.int32, shape, 0)
    lane = lax.broadcasted_iota(jnp.int32, shape, 1)
    row_lane = lax.broadcasted_iota(jnp.int32, (1, shape[1]), 1)
    info = jnp.zeros(shape, jnp.float32)
    own_sums = jnp.zeros((1, shape[1]), jnp.float32)
    for copy in fetch_small:
        copy.wait()
    for j in range(SEQ_DEV):
        group, given = group_ref[0, j], reward_ref[0, j]
        info = jnp.where((line == j) & (lane == group), 1.0, info)
        info = jnp.where(line == SEQ_DEV + j, given, info)
        for n, value in enumerate((1.0, given, given * given)):
            own_sums = own_sums + jnp.where(row_lane == n * groups + group, value, 0.0)
    info_own[...] = info
    small[0] = own_sums
    token_own[...] = jnp.zeros_like(token_own)
    with jax.named_scope('w_barrier'):
        pl.semaphore_wait(barrier, everyone - 1)

    stats = to_all(small.at[0], stat_in, 0)
    sent_out = n_rep // 2 + given_out
    mate_copies = [
        copy_to(src, dst, mate, sent_out + n, numbered()) for n, (src, dst) in enumerate((
            (info_own, info_in), (hidden_ref.at[:, other_half], hid.at[pl.ds(toks, toks)]), (cot_ref, cot.at[1]),
            (token_own, token_in)))]
    mate_info, mate_hid, mate_cot, mate_tok = mate_copies
    for copy in mate_copies[:3]:
        copy.start()

    def block(z, xx, yy):
        return roll_ref.at[pl.ds(1, layer_count - 1), span((2 * z + xx) * rows + (2 * yy + core) * sub, sub), :]

    near = [zi]
    for e in range(1, z_count):
        z = zi
        for bit in range(z_count.bit_length() - 1):
            if e >> bit & 1:
                z = flip(z, bit)[0]
        near.append(z)
    beside = (r, flip(s, 0)[0])
    above = (flip(r, 1)[0], s)
    halves_at = [yi, 1 - yi]
    m1 = [[numbered() for _ in range(1, z_count)] for _ in range(both)]

    def master_in(n, e):
        return landing(block(zi, x, halves_at[n]), m1[n][e - 1])

    def stage_masters(n):
        with jax.named_scope('w_stage'):
            fetch_stage[n].wait()
        for h in range(KV_HEADS):
            low = KV_HEADS * HEAD + h * HEAD
            for l in range(layer_count - 1):
                stage_out[n, h, l, :, :HEAD] = stage_in[n, l, :, h * HEAD:(h + 1) * HEAD].astype(jnp.bfloat16)
                stage_out[n, h, l, :, HEAD:] = stage_in[n, l, :, low:low + HEAD].astype(jnp.bfloat16)
        roll_ref[1:, span((2 * zi + x) * rows + quarters[n] * sub, sub), :] = stage_out[n, head]

    def send_masters(n, which):
        for e in which:
            put(stage_out.at[n, near[e] % KV_HEADS], block(zi, x, halves_at[n]), (r, near[e] * 2 + x),
                MASTERS, m1[n][e - 1])

    stage_masters(0)
    send_masters(0, range(1, z_count))
    spread_in = [numbered() for _ in range(z_count)]

    def second_block(e, device):
        here = block(near[e], x, 1 - yi)
        put(here, here, device, FORWARD, FORWARD)

    def spread_block(e):
        if e:
            with jax.named_scope(f'w_m1#{e}'):
                master_in(0, e).wait_recv()
        here = block(near[e], x, yi)
        put(here, here, beside, SPREAD, spread_in[e])
        put(here, here, mate, TO_MATE, TO_MATE)

    def forward_block(e, up):
        got = block(near[e], 1 - x, yi)
        with jax.named_scope(f'w_sp#{e}'):
            landing(got, spread_in[e]).wait_recv()
        if up:
            @pl.when(core == 0)
            def _():
                put(got, got, above, FORWARD, FORWARD)
        put(got, got, mate, TO_MATE, TO_MATE)

    spread_block(0)

    for copy in fetch_tokens:
        copy.wait()
    terms = token_rows(ids_in[0:1], ids_in[1:2], logp_in[0:1], logp_in[1:2], logp_in[2:3])
    for j, row in enumerate(terms):
        token_own[j:j + 1, :toks] = row
    mate_tok.start()
    if both == 2:
        stage_masters(1)
        second_block(0, beside)

    is_home = home_z == zi
    fetch_m0.wait()

    @pl.when(is_home)
    def _():
        at = span(home_piece * final, final)
        for h in range(KV_HEADS):
            low = KV_HEADS * HEAD + h * HEAD
            base_out[h, :, :HEAD] = m0[at, h * HEAD:(h + 1) * HEAD].astype(jnp.bfloat16)
            base_out[h, :, HEAD:] = m0[at, low:low + HEAD].astype(jnp.bfloat16)
        for d in range(1, z_count):
            put(base_out.at[(head + d) % KV_HEADS], base_in, z_peers[d], BASE, BASE)
        base_in[...] = base_out[head]

    with jax.named_scope('w_hid'):
        fetch_hid.wait()
        mate_hid.wait_recv()

    @pl.loop(0, half // WIDE)
    def _(t):
        at = pl.multiple_of(t * WIDE, WIDE)
        hid_t[pl.ds(at, WIDE), :] = jnp.transpose(hid[:, pl.ds(at, WIDE)])

    with jax.named_scope('w_cot'):
     fetch_cot.wait()
    mate_cot.wait_recv()
    mate_info.wait_recv()
    mate_tok.wait_recv()
    with jax.named_scope('w_stats'):
        stats.wait_recv()
    total = own_sums + jnp.sum(stat_in[...], axis=0)
    wide = shape[1]
    count = jnp.maximum(total, 1.0)
    mean = pltpu.roll(total, wide - groups, 1) / count
    spread_of = jnp.maximum(
        jnp.sqrt(jnp.maximum(pltpu.roll(total, wide - 2 * groups, 1) / count - mean * mean, 0.0)), 0.5)

    def coef_of(told, token):
        hots, given = told[:SEQ_DEV], told[SEQ_DEV:, 0:1]
        advantage = (given - jnp.sum(hots * mean, axis=1, keepdims=True)) / jnp.sum(
            hots * spread_of, axis=1, keepdims=True)
        out = token[SEQ_DEV:SEQ_DEV + 1]
        for j in range(SEQ_DEV):
            out = out + token[j:j + 1] * advantage[j:j + 1]
        return jnp.transpose(jnp.broadcast_to(out, (LANES, out.shape[1])))[:toks]

    coefs = [coef_of(info, token_own[...]), coef_of(info_in[...], token_in[...])]

    lens, offsets = [half], [0]
    for i in range(dims):
        lens.append(lens[-1] // 2)
        offsets.append(offsets[-1] + bits[i] * lens[-1])
    starts, at = [], 0
    for length in lens[1:]:
        starts.append(at)
        at += length
    turns = [2, 1, 3, 0]
    order = [(head + d) % KV_HEADS for d in turns]
    paired = z_count == KV_HEADS
    pair_z = flip(zi, 0)[0]
    inner_plane = (zi + 1) // 2 % 2 == 1
    if paired:
        outer_z = (1 - zi // 2) * 3
        order = [outer_z, flip(outer_z, 0)[0], pair_z, zi]
    tile = half // 2
    chunks = 2 * KV_HEADS
    inbound = {(i, k): numbered() for i in range(dims) for k in range(chunks)}

    def halves(i, k):
        gone = offsets[i] + (1 - bits[i]) * lens[i + 1]
        return pltpu.make_async_remote_copy(
            src_ref=part.at[order[k // 2], k % 2, span(gone, lens[i + 1])],
            dst_ref=sums.at[order[k // 2], k % 2, pl.ds(starts[i], lens[i + 1])],
            send_sem=set_send.at[HALVES], recv_sem=set_recv.at[inbound[i, k]],
            device_id=partners[i], device_id_type=MESH)

    def pass_on(i, k):
        halves(i, k).start()

    def multiply_at(h, top, n):
        where = [[[spot(j, c) for j in range(n_rep)].index(b * (n_rep // 2) + n) for b in range(2)] for c in range(2)]
        (a, b), (a1, b1) = where
        low, high = a + core * (a1 - a), b + core * (b1 - b)
        out = jnp.dot(
            hid_t[span((low + top * (high - low)) * final, final), :], delta[...], preferred_element_type=jnp.float32
        ).astype(jnp.bfloat16)
        at = span((top * (n_rep // 2) + n) * final, final)
        for side in range(2):
            part[h, side, at, :] = out[:, side * HEAD:(side + 1) * HEAD]

    for k in range(KV_HEADS):
        h = order[k]
        for side in range(2):
            low = pl.ds(pl.multiple_of(side * KV_HEADS * HEAD + h * HEAD, HEAD), HEAD)
            for src in range(2):
                delta[src * toks:(src + 1) * toks, side * HEAD:(side + 1) * HEAD] = (
                    coefs[src] * cot[src, :, low].astype(jnp.float32)).astype(jnp.bfloat16)
        if k == 0:
            for stays in (0, 1):
                for n in range(n_rep // 2):
                    multiply_at(h, bits[0] if stays else 1 - bits[0], n)
                if not stays:
                    pass_on(0, 0)
                    pass_on(0, 1)
            continue
        for t in range(2):
          with jax.named_scope(f'mul#k={k}'):
            out = jnp.dot(
                hid_t[t * tile:(t + 1) * tile, :], delta[...], preferred_element_type=jnp.float32
            ).astype(jnp.bfloat16)
            for q in range(tile // final):
                j = t * (tile // final) + q
                place = spot(j, 0) + core * (spot(j, 1) - spot(j, 0))
                for side in range(2):
                    part[h, side, span(place * final, final), :] = (
                        out[q * final:(q + 1) * final, side * HEAD:(side + 1) * HEAD])
        pass_on(0, 2 * k)
        pass_on(0, 2 * k + 1)
    spread_block(1)
    if both == 2:
        send_masters(1, [e for e in range(1, z_count) if e != 2])

    inner = min(final, 112)

    def add_in(i, k):
        h, side = order[k // 2], k % 2

        @pl.loop(0, lens[i + 1] // inner)
        def _(t):
            at = span(offsets[i + 1] + t * inner, inner)
            part[h, side, at, :] = (
                part[h, side, at, :].astype(jnp.float32)
                + sums[h, side, span(starts[i] + t * inner, inner), :].astype(jnp.float32)
            ).astype(jnp.bfloat16)

    last = dims - 1
    mine = span(offsets[dims], final)
    sources = range(2) if paired else range(z_count - 1)
    z_in = {(n, side): numbered() for side in range(2) for n in sources}
    z_mid = [numbered() for _ in range(4)] if paired else []

    def z_put(k, landing_ref, number, z):
        put(part.at[order[k // 2], k % 2, mine], landing_ref, (r, 2 * z + x), GRADS, number)

    def z_send(k):
        if not paired:
            for d in range(1, z_count):
                if d % KV_HEADS == turns[k // 2]:
                    z_put(k, zin.at[d - 1, k % 2], z_in[d - 1, k % 2], (zi + d) % z_count)
        elif k < 4:
            @pl.when(jnp.logical_not(inner_plane))
            def _():
                z_put(k, zin.at[3 + k // 2, k % 2], z_mid[k], pair_z)
        elif k < 6:
            z_put(k, zin.at[1, k % 2], z_in[1, k % 2], pair_z)

    def z_combine(k):
        held = zin.at[3 + k // 2, k % 2]

        @pl.when(inner_plane)
        def _():
            with jax.named_scope(f'w_mid#{k}'):
                landing(held, z_mid[k]).wait_recv()
            h, side = order[k // 2], k % 2
            part[h, side, mine, :] = (
                part[h, side, mine, :].astype(jnp.float32) + held[...].astype(jnp.float32)).astype(jnp.bfloat16)
            z_put(k, zin.at[0, k % 2], z_in[0, k % 2], order[k // 2])

    far = z_count > KV_HEADS
    squares = {}

    def own_sum(side):
        for n in sources:
            with jax.named_scope(f'w_z#{n}'):
                landing(zin.at[n, side], z_in[n, side]).wait_recv()
        g = part[head, side, mine, :].astype(jnp.float32)
        if not far:
            g = g + sums[head, side, pl.ds(starts[last], final), :].astype(jnp.float32)
        for n in sources:
            g = g + zin[n, side].astype(jnp.float32)
        cut = slice(side * HEAD, (side + 1) * HEAD)
        grad[:, cut] = g
        grad_b[:, cut] = g.astype(jnp.bfloat16)
        squares[side] = jnp.sum(g * g, axis=0, keepdims=True)

    for t in range(chunks + last):
        if t == chunks + last - 1:
            for e in range(2, z_count):
                spread_block(e)
            if both == 2:
                master_in(1, 1).wait_recv()

                @pl.when(core == 1)
                def _():
                    second_block(1, beside)
            forward_block(1, both == 2)
        for k in range(4 if paired else 0):
            if t == last + (3, 4, 5, 5)[k]:
                z_combine(k)
        for i in range(dims):
            k = t - i
            if k < 0 or k >= chunks:
                continue
            with jax.named_scope(f'w_in#i={i}#k={k}'):
                halves(i, k).wait_recv()
            if i == last and k // 2 == KV_HEADS - 1 and not far:
                own_sum(k % 2)
                continue
            add_in(i, k)
            if i < last:
                pass_on(i + 1, k)
            else:
                z_send(k)
        if both == 2 and t == 6 and z_count > 2:
            send_masters(1, [2])
        if t == 5:
            forward_block(0, False)
    if far:
        for side in range(2):
            own_sum(side)
    own_square = squares[0] + squares[1]
    own_square = jnp.broadcast_to(jnp.sum(own_square, axis=1, keepdims=True), (1, LANES))
    small[1, :, :LANES] = own_square
    all_squares = to_all(small.at[1, :, pl.ds(0, LANES)], square_in, 2)

    relayed = n_rep == 4 and pieces == 1
    relay_at = [numbered(), numbered()]
    y_other = flip(y, 0)[0] if relayed else y
    other_z = home(y_other)[0]
    nm_in = [numbered() for _ in range(KV_HEADS * pieces)][0]
    here_rows = rows_in.at[head, span(home_piece * final, final)]
    if relayed:
        for u in range(2):
            cut = pl.ds(u * (final // 2), final // 2)
            put(grad_b.at[cut], relay_in.at[cut], above, RELAY, relay_at[u])
        nm_copies = [
            (home_z != zi, copy_to(grad_b, here_rows, (r, 2 * home_z + x), RETURN, nm_in + head)),
            (other_z != zi, copy_to(relay_in, here_rows, (r, 2 * other_z + x), RETURN + 1, nm_in + head))]
        relay_out = [
            copy_to(relay_in.at[pl.ds(u * (final // 2), final // 2)],
                    rows_in.at[head, pl.ds(u * (final // 2), final // 2)],
                    (r, 2 * other_z + x), RETURN + 1, nm_in + head)
            for u in range(2)]
        pl.when(home_z != zi)(nm_copies[0][1].start)
    else:
        nm_copies = []
        for j in range(n_rep // 2):
            copy = copy_to(
                grad_b, here_rows, (2 * j + core, 2 * home_z + x),
                RETURN + j, nm_in + head * pieces + home_piece)
            leaves = (home_z // KV_HEADS == zi // KV_HEADS) & ((home_z != zi) | (j != y))
            nm_copies.append((leaves, copy))
            pl.when(leaves)(copy.start)

    @pl.when(is_home)
    def _():
        rows_in[head, span(home_piece * final, final), :] = grad_b[...]

    if both == 2:
        for e in range(2, z_count):
            with jax.named_scope(f'w_m2#{e}'):
                master_in(1, e).wait_recv()

        @pl.when(core == 1)
        def _():
            for e in range(2, min(z_count, 3)):
                second_block(e, beside)

    @pl.when(home_z != zi)
    def _():
        whole(base_in, BASE).wait_recv()

    with jax.named_scope('w_squares'):
        all_squares.wait_recv()
    square = own_square + jnp.sum(square_in[...], axis=0)
    rms = jnp.sqrt(square[:, 0:1] / (features * KV_HEADS * WIDE) + 1e-06)
    scale = 0.5 / rms
    row_me = row_of(y, x)

    @pl.loop(0, final // inner)
    def _(t):
        at = span(t * inner, inner)
        roll_ref[0, span(row_me + t * inner, inner), :] = (
            base_in[at, :].astype(jnp.float32) - scale * grad[at, :]).astype(jnp.bfloat16)

    parts = 4 if final // 4 % SUB == 0 else 1
    size = final // parts
    level_in = [[numbered() for _ in range(parts)] for _ in range(dims)]

    def layer0(yy, xx, u):
        return roll_ref.at[0, span(row_of(yy, xx) + u * size, size), :]

    def gather_in(i, u):
        return landing(roll_ref.at[0, pl.ds(0, size << (dims - 1 - i)), :], level_in[i][u])

    def gather_out(i, u, early=False):
        for at in have[:1] if early else have[int(i == 0 < last):1 << (last - i)]:
            here = layer0(*at, u)
            put(here, here, partners[i], GATHER, level_in[i][u])

    def piece_out(at):
        for u in range(parts):
            here = layer0(*at, u)
            put(here, here, mate, PIECES, PIECES)

    have = [(y, x)]
    for i in reversed(range(dims)):
        have = have + [across(*at, i) for at in have]
    for u in range(parts):
        gather_out(last, u)
    for u in range(parts if last else 0):
        gather_out(0, u, True)
    piece_out(have[0])
    if relayed:
        for u in range(2):
            with jax.named_scope('w_relay'):
                landing(relay_in.at[pl.ds(u * (final // 2), final // 2)], relay_at[u]).wait_recv()
            pl.when(other_z != zi)(relay_out[u].start)

        @pl.when(other_z == zi)
        def _():
            rows_in[head] = relay_in[...]
    for e in range(2, z_count):
        forward_block(e, both == 2)
    if both == 2:
        @pl.when(core == 1)
        def _():
            for e in range(3, z_count):
                second_block(e, beside)
    for i in reversed(range(last)):
        for u in range(parts):
            with jax.named_scope(f'w_ag#{i + 1}#{u}'):
                gather_in(i + 1, u).wait_recv()
            gather_out(i, u)
        for at in have[1 << (last - 1 - i):1 << (last - i)]:
            piece_out(at)

    keeper = zi // half_z
    hand_in = [numbered() for _ in range(KV_HEADS)]
    hand_over = [copy_to(rows_in.at[h], rows_in.at[h], mate, HAND, hand_in[h]) for h in range(KV_HEADS)]

    def landed(h, p):
        return landing(rows_in.at[h, pl.ds(p * final, final)], nm_in + h * pieces + p)

    @pl.when(core == keeper)
    @jax.named_scope('w_rows')
    def _():
        low = zi + core * (z_count - 1 - 2 * zi)
        for h in range(KV_HEADS):
            for p in range(pieces):
                @pl.when((h != head) if relayed else (h != head) | (y != low * pieces + p))
                def _():
                    landed(h, p).wait_recv()
            hand_over[h].start()

    blocks = roll_ref.at[pl.ds(1, layer_count - 1), pl.ds(0, z_count * sub), :]
    if both == 2:
        with jax.named_scope('w_fwd'):
            whole(blocks, FORWARD).wait_recv()
        for z in near:
            for xx in (x, 1 - x):
                got = block(z, xx, 1 - yi)
                put(got, got, mate, TO_MATE, TO_MATE)
    @pl.when(core != keeper)
    @jax.named_scope('w_hand')
    def _():
        for copy in hand_over:
            copy.wait_recv()

    for h in range(KV_HEADS):
        for side in range(2):
            low = side * KV_HEADS * HEAD + h * HEAD
            nm_ref[:, low:low + HEAD] = (
                m0[:, low:low + HEAD] - scale * rows_in[h, :, side * HEAD:(side + 1) * HEAD].astype(jnp.float32))

    @pl.when(is_home)
    def _():
        whole(zin.at[pl.ds(0, z_count - 1)], BASE).wait_send()

    for leaves, copy in nm_copies:
        pl.when(leaves)(copy.wait_send)
    for copy in mate_copies:
        copy.wait_send()
    whole(roll_ref.at[pl.ds(1, layer_count - 1), pl.ds(0, (z_count - 1) * both * sub), :], MASTERS).wait_send()
    whole(blocks, SPREAD).wait_send()
    if relayed:
        whole(relay_in, RELAY).wait_send()
    whole(part.at[:, :, pl.ds(0, half - final), :], HALVES).wait_send()
    whole(zin.at[pl.ds(0, z_count - 1)], GRADS).wait_send()
    stats.wait_send()
    all_squares.wait_send()
    with jax.named_scope('w_gathered'):
        for u in range(parts):
            gather_in(0, u).wait_recv()
            for at in have[n_rep // 2:]:
                here = layer0(*at, u)
                put(here, here, mate, PIECES, PIECES)

    all_blocks = roll_ref.at[pl.ds(1, layer_count - 1), pl.ds(0, z_count * split * sub), :]
    all_pieces = roll_ref.at[0, pl.ds(0, n_rep * final), :]
    with jax.named_scope('w_mate'):
        whole(all_blocks, TO_MATE).wait_recv()
        whole(all_pieces, PIECES).wait_recv()

    @pl.when(core == keeper)
    def _():
        whole(rows_in, HAND).wait_send()

    if both == 2:
        whole(blocks, FORWARD).wait_send()
    whole(all_blocks, TO_MATE).wait_send()
    whole(all_pieces, PIECES).wait_send()
    whole(roll_ref.at[0, pl.ds(0, (n_rep - 1) * final), :], GATHER).wait_send()


def copy_kernel(nm_ref, roll_ref, nm_out, roll_out, sems):
    layer_count, features, _ = roll_ref.shape
    copies = [pltpu.make_async_copy(nm_ref, nm_out, sems.at[0])]
    for l in range(layer_count):
        for n in range(2):
            cut = pl.ds(n * (features // 2), features // 2)
            copies.append(pltpu.make_async_copy(
                roll_ref.at[l, cut], roll_out.at[l, cut], sems.at[1 + 2 * l + n]))
    for copy in copies:
        copy.start()
    for copy in copies:
        copy.wait()


def per_device(
    n_rep, n_shard, hidden, cotangent, seq_ids, response_mask, group_ids, rewards, new_logp, old_logp, ref_logp,
    master,
):
    everyone = n_rep * n_shard
    groups = everyone * SEQ_DEV // 8
    wide = -(-3 * groups // LANES) * LANES
    toks, features = hidden.shape
    layer_count, rows, cols = master.shape
    z_count = n_shard // 2
    split = 4 if n_rep % 4 == 0 and (rows // 4) % SUB == 0 else 2
    sub = rows // split
    half = features // 2
    final = half // n_rep
    pad = -(-toks // LANES) * LANES
    bf16, f32 = jnp.bfloat16, jnp.float32
    vmem, hbm = pl.BlockSpec(memory_space=pltpu.VMEM), pl.BlockSpec(memory_space=pltpu.HBM)
    dims = n_rep.bit_length() - 1
    both = 2 if split == 4 else 1
    landings = 7 + 4 + 2 + 4 + KV_HEADS + both * (z_count - 1) + z_count + 8 * dims + 2 * (z_count - 1) + KV_HEADS * (n_rep // z_count) + 4 * dims
    results = pl.pallas_call(
        functools.partial(step_kernel, n_rep, n_shard, split, groups),
        out_shape=(pltpu.VMEM((rows, cols), f32), pltpu.VMEM((layer_count, features, WIDE), bf16)),
        in_specs=[hbm] * 10,
        out_specs=(vmem, vmem),
        scratch_shapes=[
            pltpu.SMEM((1, SEQ_DEV), jnp.int32),
            pltpu.SMEM((1, SEQ_DEV), f32),
            pltpu.VMEM((2, toks), jnp.int32),
            pltpu.VMEM((3, toks), f32),
            pltpu.VMEM((2, 1, wide), f32),
            pltpu.VMEM((everyone - 1, 1, wide), f32),
            pltpu.VMEM((everyone - 1, 1, LANES), f32),
            pltpu.VMEM((8, wide), f32),
            pltpu.VMEM((8, wide), f32),
            pltpu.VMEM((8, pad), f32),
            pltpu.VMEM((8, pad), f32),
            pltpu.VMEM((2 * toks, half), bf16),
            pltpu.VMEM((half, 2 * toks), bf16),
            pltpu.VMEM((2, toks, cols), bf16),
            pltpu.VMEM((2 * toks, WIDE), bf16),
            pltpu.VMEM((KV_HEADS, 2, half, HEAD), bf16),
            pltpu.VMEM((KV_HEADS, 2, half, HEAD), bf16),
            pltpu.VMEM((z_count + 1, 2, final, HEAD), bf16),
            pltpu.VMEM((final, WIDE), f32),
            pltpu.VMEM((final, WIDE), bf16),
            pltpu.VMEM((final, WIDE), bf16),
            pltpu.VMEM((KV_HEADS, final, WIDE), bf16),
            pltpu.VMEM((final, WIDE), bf16),
            pltpu.VMEM((rows, cols), f32),
            pltpu.VMEM((2, layer_count - 1, sub, cols), f32),
            pltpu.VMEM((2, KV_HEADS, layer_count - 1, sub, WIDE), bf16),
            pltpu.VMEM((KV_HEADS, rows, WIDE), bf16),
            pltpu.SemaphoreType.DMA((12,)),
            pltpu.SemaphoreType.DMA((4,)),
            pltpu.SemaphoreType.DMA((16 + n_rep // 2,)),
            pltpu.SemaphoreType.DMA((landings,)),
        ],
        compiler_params=pltpu.CompilerParams(
            collective_id=0, has_side_effects=True, vmem_limit_bytes=44 * 2**20
        ),
        name="step",
    )(*(pltpu.with_memory_space_constraint(value, pltpu.HBM) for value in (
        group_ids, rewards, seq_ids, response_mask, new_logp, old_logp, ref_logp, hidden, cotangent, master)))
    return pl.pallas_call(
        copy_kernel,
        out_shape=tuple(jax.ShapeDtypeStruct(value.shape, value.dtype) for value in results),
        in_specs=[vmem] * 2,
        out_specs=(hbm, hbm),
        scratch_shapes=[pltpu.SemaphoreType.DMA((8,))],
        compiler_params=pltpu.CompilerParams(vmem_limit_bytes=2**20),
        name="copy",
    )(*(pltpu.with_memory_space_constraint(value, pltpu.VMEM) for value in results))


def solution(mesh):
    tokens = P(("rep", "shard"), None)
    return jax.shard_map(
        functools.partial(per_device, mesh.shape["rep"], mesh.shape["shard"]),
        mesh=mesh,
        in_specs=(tokens,) * 9 + (P(None, "shard", None),),
        out_specs=(P("shard", None), P(None, None, "shard")),
        check_vma=False,
    )
```
